32 devices in a mesh: dp: 2 (over x), seq: 16 (over z, y, core).
Axes of the slice: x: 2, y: 2, z: 4, core: 2. Of those that a mesh axis runs over, the one named last changes fastest.
Arguments:
- grad_out: bfloat16 [2, 4096, 512], P('dp', 'seq'), may hold values from -6 to 6
- gate: bfloat16 [2, 4096, 512], P('dp', 'seq'), may hold values from -6 to 6
- signal: bfloat16 [2, 4096, 512], P('dp', 'seq'), may hold values from -6 to 6
- filters: float32 [2, 256, 4096], P(None, 'seq', 'dp'), may hold values from -0.09375 to 0.09375
Outputs:
- grad_signal: bfloat16 [2, 4096, 512], P('dp', 'seq')
- grad_gate: bfloat16 [2, 4096, 512], P('dp', 'seq')
- grad_filter: float32 [2, 256, 4096], P(None, 'seq', 'dp')
The draws below stay inside these ranges and needn't reach their ends.
All inputs are finite; a program needn't handle non-finite values.
Results may differ from the reference program's by a relative error of at most 0.005.
Values may be sent and summed in bfloat16 or wider, within the bound.
No kernel may reach another device: no remote copies, remote signals or barrier semaphores. Data moves between devices by JAX's collectives and lax.ppermute only.
A program may use at most 128 MiB of HBM per device.

```python
import jax
import jax.numpy as jnp

SEG_CH = 256
SEGMENTS = 2
LEN = 4096
BATCH = 2


def block_levels(key, dims, split, smallest, high):
    def one(dim, shards_of):
        draws = jax.random.uniform(jax.random.fold_in(jax.random.fold_in(key, 6), dim), (shards_of,), jnp.float32, smallest / len(split), high / len(split))
        return jnp.repeat(jnp.exp(draws), dims[dim] // shards_of).reshape((-1,) + (1,) * (len(dims) - dim - 1))

    factor_of = one(*split[0])
    for cut in split[1:]:
        factor_of = factor_of * one(*cut)
    return factor_of


def noise(rng, extent, width, limit, shards=(), dtype=jnp.bfloat16):
    result = width * jax.random.normal(rng, extent, jnp.float32)
    if shards:
        result = result * block_levels(rng, extent, shards, -0.22, 0.18)
    return jnp.clip(result, -limit, limit).astype(dtype)


def setup_inputs(seed: int = 0) -> dict:
    arg_keys = jax.random.split(jax.random.key(seed), 5)
    grad_out = noise(arg_keys[0], (BATCH, LEN, SEGMENTS * SEG_CH), 1.0, 6.0, ((0, 2), (1, 16)))
    gate = noise(arg_keys[1], (BATCH, LEN, SEGMENTS * SEG_CH), 1.0, 6.0, ((0, 2), (1, 16)))
    signal = noise(arg_keys[2], (BATCH, LEN, SEGMENTS * SEG_CH), 1.0, 6.0, ((0, 2), (1, 16)))
    filters = noise(arg_keys[3], (SEGMENTS, SEG_CH, LEN), LEN ** -0.5, 0.09375, ((1, 16), (2, 2)), jnp.float32)
    return dict(grad_out=grad_out, gate=gate, signal=signal, filters=filters)


def forward_spectrum(values):
    return jnp.fft.rfft(values, n=2 * values.shape[-1], axis=-1)


def back_values(spectrum, length):
    return jnp.fft.irfft(spectrum, n=2 * length, axis=-1)[..., :length]


def reference(grad_out, gate, signal, filters):
    channels = SEGMENTS * SEG_CH
    gradient = grad_out.astype(jnp.float32)
    scaled = (gradient * gate.astype(jnp.float32)).astype(jnp.bfloat16)
    scaled_rows = jnp.transpose(scaled.astype(jnp.float32), (0, 2, 1))
    signal_rows = jnp.transpose(signal.astype(jnp.float32), (0, 2, 1))
    filter_spectrum = forward_spectrum(filters.reshape(channels, LEN))
    signal_spectrum = forward_spectrum(signal_rows)
    scaled_spectrum = forward_spectrum(scaled_rows)
    convolved = back_values(filter_spectrum * signal_spectrum, LEN).astype(jnp.bfloat16)
    adjoint = back_values(jnp.conj(filter_spectrum) * scaled_spectrum, LEN)
    kernels = back_values(scaled_spectrum * jnp.conj(signal_spectrum), LEN)
    grad_signal = jnp.transpose(adjoint, (0, 2, 1)).astype(jnp.bfloat16)
    conv_tokens = jnp.transpose(convolved, (0, 2, 1)).astype(jnp.float32)
    grad_gate = (gradient * conv_tokens).astype(jnp.bfloat16)
    factor = (BATCH * LEN) ** -0.5
    grad_filter = (jnp.sum(kernels, axis=0) * factor).reshape(SEGMENTS, SEG_CH, LEN)
    return grad_signal, grad_gate, grad_filter
```

```python
import functools

import jax
import jax.numpy as jnp
from jax import lax
from jax.experimental import pallas as pl
from jax.experimental.pallas import tpu as pltpu
from jax.sharding import PartitionSpec as P

LANES = 128
bf16 = jnp.bfloat16
f32 = jnp.float32


def iota(shape, axis):
    return lax.broadcasted_iota(jnp.int32, shape, axis)


def flip_matrix(size, dtype):
    hit = iota((size, size), 0) + iota((size, size), 1) == size - 1
    return jnp.where(hit, 1.0, 0.0).astype(dtype)


def times(a, b):
    return jnp.dot(a, b, preferred_element_type=f32)


def gather_rows(parts):
    return parts[0] if len(parts) == 1 else jnp.concatenate(parts, axis=0)


def loop(count, body, unrolled):
    if unrolled:
        for i in range(count):
            body(i)
    else:
        lax.fori_loop(0, count, lambda i, _: (body(i), 0)[1], 0)


def send_kernel(sizes, out_grad, gate, signal, sent):
    dp, seq, per, spd = sizes
    scaled = (out_grad[...].astype(f32) * gate[...].astype(f32)).astype(bf16)
    width = per * seq
    for p in range(dp):
        turned = []
        for value in (scaled, signal[...]):
            for s in range(spd):
                begin = (p * spd + s) * width
                turned.append(value[:, begin : begin + width].astype(f32).T)
        for q in range(seq):
            rows = gather_rows([t[q * per : (q + 1) * per] for t in turned])
            sent[p * seq + q] = rows.astype(bf16)


def receive_kernel(sizes, got, out_grad, grad_signal, grad_gate):
    dp, seq, per, spd = sizes
    width = per * seq
    cpd = per * spd
    for p in range(dp):
        for s in range(spd):
            begin = (p * spd + s) * width
            turned = []
            for t in range(2):
                low = t * cpd + s * per
                block = got[p * seq : (p + 1) * seq].astype(f32)
                turned.append(gather_rows([block[q, low : low + per] for q in range(seq)]).T)
            grad = out_grad[:, begin : begin + width].astype(f32)
            grad_gate[:, begin : begin + width] = (grad * turned[0]).astype(bf16)
            grad_signal[:, begin : begin + width] = turned[1].astype(bf16)


def stage_flipped(dp, seq, cpd, got, held):
    tokens = got.shape[2]
    flip = flip_matrix(tokens, bf16)
    for b in range(dp):
        block = got[b * seq : (b + 1) * seq, :cpd].reshape(seq * cpd, tokens)
        turned = times(block, flip)
        for q in range(seq):
            to = pl.ds((b * seq + seq - 1 - q) * cpd, cpd)
            for half in range(tokens // LANES):
                held[half, to, :] = turned[q * cpd : (q + 1) * cpd, half * LANES : (half + 1) * LANES]


def filter_row(taps, c, d):
    per_part = taps.shape[2]
    return taps[d // per_part, c, pl.ds(d % per_part, 1), :]


def skew(row):
    return pltpu.roll(jnp.broadcast_to(row, (LANES, LANES)), 0, 1, stride=1, stride_axis=0)


def mix_kernel(sizes, got, taps, made, plain, turned, padded, result, out):
    dp, seq, cpd = sizes
    tokens = got.shape[2]
    halves = tokens // LANES
    blocks = seq * halves
    streams = [(kind, b) for kind in range(2) for b in range(dp)]
    rows = dp * seq * cpd
    value = got[:, cpd:].astype(f32).reshape(rows, tokens)
    for half in range(halves):
        plain[half] = value[:, half * LANES : (half + 1) * LANES]
    stage_flipped(dp, seq, cpd, got, turned)
    for s in range(len(streams)):
        padded[s, :blocks] = jnp.zeros((blocks, LANES), f32)
    lower = iota((LANES, LANES), 1) >= iota((LANES, LANES), 0)
    held = (plain, turned)

    def channel(c, carry):
        for s, (kind, b) in enumerate(streams):
            for half in range(halves):
                from_rows = pl.ds(b * seq * cpd + c, seq, stride=cpd)
                padded[s, pl.ds(blocks + half, seq, stride=halves), :] = held[kind][half, from_rows, :]
        before = jnp.zeros((LANES, LANES), f32)
        total = [None, None]
        for e in range(blocks // 2):
            tiles = []
            for d in (2 * e, 2 * e + 1):
                now = skew(filter_row(taps, c, d))
                tiles.append(jnp.where(lower, now, before).astype(bf16))
                before = now
            first = 0 if 4 * e < blocks else blocks // 2
            count = blocks - first
            left = []
            for d in (2 * e, 2 * e + 1):
                at = pl.ds(blocks + first - d, count)
                left.append(jnp.concatenate([padded[s, at, :] for s in range(len(streams))], axis=0))
            left = jnp.concatenate(left, axis=1).astype(bf16)
            product = times(left, jnp.concatenate(tiles, axis=0))
            which = 0 if first == 0 else 1
            total[which] = product if total[which] is None else total[which] + product
        half_blocks = blocks // 2
        for s, (kind, b) in enumerate(streams):
            whole = total[0][s * blocks : (s + 1) * blocks]
            result[s, :half_blocks] = whole[:half_blocks]
            result[s, half_blocks:] = whole[half_blocks:] + total[1][s * half_blocks : (s + 1) * half_blocks]
            for half in range(halves):
                to_rows = pl.ds(b * seq * cpd + c, seq, stride=cpd)
                out[kind, half, to_rows, :] = result[s, pl.ds(half, seq, stride=halves), :]
        return carry

    lax.fori_loop(0, cpd, channel, 0)
    flip = flip_matrix(tokens, bf16)
    for kind in range(2):
        for b in range(dp):
            at = pl.ds(b * seq * cpd, seq * cpd)
            value = jnp.concatenate([out[kind, half, at, :] for half in range(halves)], axis=1).astype(bf16)
            if kind == 1:
                value = times(value, flip).astype(bf16)
            for q in range(seq):
                to = b * seq + (q if kind == 0 else seq - 1 - q)
                made[to, kind * cpd : (kind + 1) * cpd] = value[q * cpd : (q + 1) * cpd]


def tap_kernel(sizes, factor, got, made, mirrored, turned, padded, delayed, square, partial, lags):
    dp, seq, cpd = sizes
    tokens = got.shape[2]
    halves = tokens // LANES
    blocks = seq * halves
    small = LANES // 2
    stage_flipped(dp, seq, cpd, got, turned)
    for b in range(dp):
        for q in range(seq):
            block = got[b * seq + q].astype(f32)[cpd:]
            to = pl.ds((b * seq + seq - 1 - q) * cpd, cpd)
            for half in range(halves):
                mirrored[halves - 1 - half, to, :] = block[:, half * LANES : (half + 1) * LANES]
    for b in range(dp):
        padded[b, :blocks] = jnp.zeros((blocks, LANES), f32)
        delayed[b, :blocks] = jnp.zeros((blocks, LANES), f32)
    low_half = iota((blocks, LANES), 1) < small
    lower = iota((small, LANES), 1) >= iota((small, LANES), 0)

    def channel(c, carry):
        for b in range(dp):
            for half in range(halves):
                rows = pl.ds(b * seq * cpd + c, seq, stride=cpd)
                padded[b, pl.ds(blocks + half, seq, stride=halves), :] = turned[half, rows, :]
                square[b, pl.ds(half, seq, stride=halves), :] = mirrored[half, rows, :]
        for b in range(dp):
            here = pltpu.roll(padded[b, blocks:], small, 1)
            behind = pltpu.roll(padded[b, pl.ds(blocks - 1, blocks), :], small, 1)
            delayed[b, blocks:] = jnp.where(low_half, behind, here)
        wide = jnp.concatenate([square[b] for b in range(dp)], axis=0).T
        left = jnp.concatenate([wide[:small], wide[small:]], axis=1).astype(bf16)
        before = jnp.zeros((small, LANES), f32)
        for pair in range(blocks // 2):
            right = []
            for at in (2 * pair, 2 * pair + 1):
                rows = pl.ds(at + 1, blocks)
                parts = [padded[b, rows, :] for b in range(dp)] + [delayed[b, rows, :] for b in range(dp)]
                right.append(jnp.concatenate(parts, axis=0).astype(bf16))
            product = times(left, jnp.concatenate(right, axis=1))
            for k in range(2):
                now = pltpu.roll(product[:, k * LANES : (k + 1) * LANES], 0, 1, stride=1, stride_axis=0)
                value = jnp.where(lower, now, before)
                before = now
                value = jnp.sum(value.reshape(small // 8, 8, LANES), axis=0)
                partial[pl.ds((2 * pair + k) * 8, 8), :] = value
        total = partial[pl.ds(0, blocks, stride=8), :]
        for j in range(1, 8):
            total = total + partial[pl.ds(j, blocks, stride=8), :]
        lags[pl.ds(c * blocks, blocks), :] = total * factor
        return carry

    lax.fori_loop(0, cpd, channel, 0)
    flip = flip_matrix(LANES, f32)
    lags[...] = jnp.dot(lags[...], flip, preferred_element_type=f32, precision=lax.Precision.HIGHEST)
    per_part = blocks // made.shape[0]
    for k in range(blocks):
        column = pl.ds((k % per_part) * LANES, LANES)
        made[k // per_part, :, column] = lags[pl.ds(blocks - 1 - k, cpd, stride=blocks), :]


def exchange(blocks, axis):
    size = blocks.shape[0]
    me = lax.axis_index(axis)
    own = lax.dynamic_index_in_dim(blocks, me, 0, True)
    result = lax.dynamic_update_slice_in_dim(jnp.zeros_like(blocks), own, me, 0)
    for k in range(1, size):
        part = lax.dynamic_index_in_dim(blocks, (me + k) % size, 0, True)
        part = lax.ppermute(part, axis, [(i, (i + k) % size) for i in range(size)])
        result = lax.dynamic_update_slice_in_dim(result, part, (me - k) % size, 0)
    return result


def call(kernel, out_shape, scratch=(), flops=0):
    return pl.pallas_call(
        kernel,
        out_shape=out_shape,
        scratch_shapes=list(scratch),
        cost_estimate=pl.CostEstimate(flops=flops, bytes_accessed=1 << 20, transcendentals=0),
        compiler_params=pltpu.CompilerParams(vmem_limit_bytes=60000 * 1024),
    )


def on_device(grad_out, gate, signal, filters):
    shape = jax.ShapeDtypeStruct
    dp, seq = lax.axis_size("dp"), lax.axis_size("seq")
    tokens, channels = grad_out.shape[1:]
    segments, per, part = filters.shape
    spd = segments // dp
    cpd = spd * per
    length = tokens * seq
    halves = tokens // LANES
    blocks = length // LANES
    rows = dp * seq * cpd
    both = ("dp", "seq")
    taps = exchange(filters.reshape(dp, cpd, part // LANES, LANES), "dp")
    edge = (dp, seq, per, spd)
    sent = call(
        functools.partial(send_kernel, edge),
        shape((dp * seq, 2 * cpd, tokens), bf16),
    )(grad_out[0], gate[0], signal[0])
    got = lax.all_to_all(sent, both, split_axis=0, concat_axis=0, tiled=True)
    inner = (dp, seq, cpd)
    made = call(
        functools.partial(mix_kernel, inner),
        shape((dp * seq, 2 * cpd, tokens), bf16),
        (
            pltpu.VMEM((halves, rows, LANES), f32),
            pltpu.VMEM((halves, rows, LANES), f32),
            pltpu.VMEM((2 * dp, 2 * blocks, LANES), f32),
            pltpu.VMEM((2 * dp, blocks, LANES), f32),
            pltpu.VMEM((2, halves, rows, LANES), f32),
        ),
    )(got, taps)
    back = lax.all_to_all(made, both, split_axis=0, concat_axis=0, tiled=True)
    lags = call(
        functools.partial(tap_kernel, inner, float(dp * length) ** -0.5),
        shape((dp, cpd, part), f32),
        (
            pltpu.VMEM((halves, rows, LANES), f32),
            pltpu.VMEM((halves, rows, LANES), f32),
            pltpu.VMEM((dp, 2 * blocks, LANES), f32),
            pltpu.VMEM((dp, 2 * blocks, LANES), f32),
            pltpu.VMEM((dp, blocks, LANES), f32),
            pltpu.VMEM((blocks * 8, LANES), f32),
            pltpu.VMEM((cpd * blocks, LANES), f32),
        ),
        flops=1 << 30,
    )(got)
    grad_filter = exchange(lags, "dp").reshape(segments, per, part)
    grad_signal, grad_gate = call(
        functools.partial(receive_kernel, edge),
        (shape((tokens, channels), bf16), shape((tokens, channels), bf16)),
    )(back, grad_out[0])
    return (grad_signal[None], grad_gate[None], grad_filter)


def solution(mesh):
    tokens = P("dp", "seq", None)
    taps = P(None, "seq", "dp")
    return jax.shard_map(
        on_device,
        mesh=mesh,
        in_specs=(tokens, tokens, tokens, taps),
        out_specs=(tokens, tokens, taps),
        check_vma=False,
    )
```

```python
import functools

import jax
import jax.numpy as jnp
from jax import lax
from jax.experimental import pallas as pl
from jax.experimental.pallas import tpu as pltpu
from jax.sharding import PartitionSpec as P

LANES = 128
PACK = 16
AHEAD = 2
bf16 = jnp.bfloat16
f32 = jnp.float32


def iota(shape, axis):
    return lax.broadcasted_iota(jnp.int32, shape, axis)


def flip_matrix(size, dtype):
    hit = iota((size, size), 0) + iota((size, size), 1) == size - 1
    return jnp.where(hit, 1.0, 0.0).astype(dtype)


def times(a, b):
    return jnp.dot(a, b, preferred_element_type=f32)


def gather_rows(parts):
    return parts[0] if len(parts) == 1 else jnp.concatenate(parts, axis=0)


def send_kernel(sizes, out_grad, gate, signal, sent, grads, gates, signals, made, arrived, left):
    dp, seq, per, spd = sizes
    width = per * seq * spd
    pairs = ((signal, signals), (out_grad, grads), (gate, gates))
    coming = [
        [
            pltpu.make_async_copy(
                source.at[:, pl.ds(p * width, width)],
                held.at[:, pl.ds(p * width, width)],
                arrived.at[k, p],
            )
            for k, (source, held) in enumerate(pairs)
        ]
        for p in range(dp)
    ]
    going = [
        pltpu.make_async_copy(made.at[pl.ds(p * seq, seq)], sent.at[pl.ds(p * seq, seq)], left.at[p])
        for p in range(dp)
    ]
    for copies in coming:
        for copy in copies:
            copy.start()
    for p in range(dp):
        at = pl.ds(p * width, width)
        for copy in coming[p]:
            copy.wait()
        plain = signals[:, at].astype(f32).T
        scaled = (grads[:, at].astype(f32) * gates[:, at].astype(f32)).T
        for q in range(seq):
            parts = []
            for value in (scaled, plain):
                for s in range(spd):
                    begin = (s * seq + q) * per
                    parts.append(value[begin : begin + per])
            made[p * seq + q] = gather_rows(parts).astype(bf16)
        going[p].start()
    for copy in going:
        copy.wait()


def receive_kernel(sizes, got, out_grad, grad_signal, grad_gate):
    dp, seq, per, spd = sizes
    width = per * seq
    cpd = per * spd
    for p in range(dp):
        for s in range(spd):
            begin = (p * spd + s) * width
            turned = []
            for t in range(2):
                low = t * cpd + s * per
                block = got[p * seq : (p + 1) * seq].astype(f32)
                turned.append(gather_rows([block[q, low : low + per] for q in range(seq)]).T)
            grad = out_grad[:, begin : begin + width].astype(f32)
            grad_gate[:, begin : begin + width] = (grad * turned[0]).astype(bf16)
            grad_signal[:, begin : begin + width] = turned[1].astype(bf16)


def stage_flipped(dp, seq, cpd, got, held):
    tokens = got.shape[2]
    flip = flip_matrix(tokens, bf16)
    for b in range(dp):
        block = got[b * seq : (b + 1) * seq, :cpd].reshape(seq * cpd, tokens)
        turned = times(block, flip)
        for q in range(seq):
            to = pl.ds((b * seq + seq - 1 - q) * cpd, cpd)
            for half in range(tokens // LANES):
                held[half, to, :] = turned[q * cpd : (q + 1) * cpd, half * LANES : (half + 1) * LANES]


def skew(value):
    return pltpu.roll(value, 0, 1, stride=1, stride_axis=0)


def tile_kernel(taps, tiles):
    parts, cpd, per_part, _ = taps.shape
    lower = iota((LANES, LANES), 1) >= iota((LANES, LANES), 0)

    def channel(c, carry):
        before = jnp.zeros((LANES, LANES), f32)
        for d in range(parts * per_part):
            row = taps[d // per_part, c, pl.ds(d % per_part, 1), :]
            now = skew(jnp.broadcast_to(row, (LANES, LANES)))
            tiles[c, pl.ds(d * LANES, LANES), :] = jnp.where(lower, now, before).astype(bf16)
            before = now
        return carry

    lax.fori_loop(0, cpd, channel, 0)


def spread(line, shifted, u, streams, blocks):
    size = blocks * streams
    for k in range(PACK // streams):
        at = pl.ds(PACK - k * streams, size)
        shifted[u, k, size:] = line[u, at, :].astype(bf16)


def mix_kernel(sizes, got, taps, made, plain, turned, line, shifted, result, out):
    dp, seq, cpd = sizes
    tokens = got.shape[2]
    halves = tokens // LANES
    blocks = seq * halves
    streams = 2 * dp
    size = blocks * streams
    rows = dp * seq * cpd
    ahead = line.shape[0]
    value = got[:, cpd:].astype(f32).reshape(rows, tokens)
    for half in range(halves):
        plain[half] = value[:, half * LANES : (half + 1) * LANES]
    stage_flipped(dp, seq, cpd, got, turned)
    for u in range(ahead):
        line[u, :PACK] = jnp.zeros((PACK, LANES), f32)
        for k in range(PACK // streams):
            shifted[u, k, :size] = jnp.zeros((size, LANES), bf16)
    lower = iota((LANES, LANES), 1) >= iota((LANES, LANES), 0)
    held = (plain, turned)
    order = [(k, b, half) for k in range(2) for b in range(dp) for half in range(halves)]

    def channel(c, u):
        for kind, b, half in order:
            rows = pl.ds(b * seq * cpd + c, seq, stride=cpd)
            to = pl.ds(PACK + half * streams + kind * dp + b, seq, stride=halves * streams)
            line[u, to, :] = held[kind][half, rows, :]
        spread(line, shifted, u, streams, blocks)
        total = [None, None]
        before = jnp.zeros((LANES, LANES), f32)
        for e in range(blocks // 2):
            tiles = []
            for d in (2 * e, 2 * e + 1):
                row = taps[d // taps.shape[2], c, pl.ds(d % taps.shape[2], 1), :]
                now = skew(jnp.broadcast_to(row, (LANES, LANES)))
                tiles.append(jnp.where(lower, now, before).astype(bf16))
                before = now
            which = 0 if 4 * e < blocks else 1
            count = size >> which
            left = []
            for d in (2 * e, 2 * e + 1):
                k = d % (PACK // streams)
                at = 2 * size - count - (d - k) * streams
                left.append(shifted[u, k, pl.ds(at, count), :])
            product = times(jnp.concatenate(left, axis=1), jnp.concatenate(tiles, axis=0))
            total[which] = product if total[which] is None else total[which] + product
        result[u, : size // 2] = total[0][: size // 2]
        result[u, size // 2 :] = total[0][size // 2 :] + total[1]
        for kind, b, half in order:
            rows = pl.ds(b * seq * cpd + c, seq, stride=cpd)
            at = pl.ds(half * streams + kind * dp + b, seq, stride=halves * streams)
            out[kind, half, rows, :] = result[u, at, :]

    def step(i, carry):
        for u in range(ahead):
            channel(i * ahead + u, u)
        return carry

    lax.fori_loop(0, cpd // ahead, step, 0)
    flip = flip_matrix(tokens, bf16)
    for kind in range(2):
        for b in range(dp):
            at = pl.ds(b * seq * cpd, seq * cpd)
            value = jnp.concatenate([out[kind, half, at, :] for half in range(halves)], axis=1).astype(bf16)
            if kind == 1:
                value = times(value, flip).astype(bf16)
            for q in range(seq):
                to = b * seq + (q if kind == 0 else seq - 1 - q)
                made[to, kind * cpd : (kind + 1) * cpd] = value[q * cpd : (q + 1) * cpd]


def tap_kernel(sizes, factor, got, made, mirrored, turned, plain, line, shifted, square, partial, lags):
    dp, seq, cpd = sizes
    tokens = got.shape[2]
    halves = tokens // LANES
    blocks = seq * halves
    streams = 2 * dp
    size = blocks * streams
    small = LANES // 2
    ahead = line.shape[0]
    stage_flipped(dp, seq, cpd, got, turned)
    for b in range(dp):
        for q in range(seq):
            block = got[b * seq + q].astype(f32)[cpd:]
            to = pl.ds((b * seq + seq - 1 - q) * cpd, cpd)
            for half in range(halves):
                mirrored[halves - 1 - half, to, :] = block[:, half * LANES : (half + 1) * LANES]
    for u in range(ahead):
        line[u, :PACK] = jnp.zeros((PACK, LANES), f32)
        for b in range(dp):
            plain[u, b, :8] = jnp.zeros((8, LANES), f32)
        for k in range(PACK // streams):
            shifted[u, k, :size] = jnp.zeros((size, LANES), bf16)
    low_half = iota((blocks, LANES), 1) < small
    lower = iota((small, LANES), 1) >= iota((small, LANES), 0)

    def channel(c, u):
        for b in range(dp):
            for half in range(halves):
                rows = pl.ds(b * seq * cpd + c, seq, stride=cpd)
                plain[u, b, pl.ds(8 + half, seq, stride=halves), :] = turned[half, rows, :]
                value = mirrored[half, rows, :]
                for k in range(2):
                    to = pl.ds(half * streams + k * dp + b, seq, stride=halves * streams)
                    square[u, to, :] = pltpu.roll(value, small, 1) if k else value
        for b in range(dp):
            here = plain[u, b, 8:]
            behind = plain[u, b, pl.ds(7, blocks), :]
            late = jnp.where(low_half, pltpu.roll(behind, small, 1), pltpu.roll(here, small, 1))
            line[u, pl.ds(PACK + b, blocks, stride=streams), :] = here
            line[u, pl.ds(PACK + dp + b, blocks, stride=streams), :] = late
        spread(line, shifted, u, streams, blocks)
        left = square[u].T[:small].astype(bf16)
        before = jnp.zeros((small, LANES), f32)
        for pair in range(blocks // 2):
            right = []
            for at in (2 * pair + 1, 2 * pair + 2):
                k = -at % (PACK // streams)
                right.append(shifted[u, k, pl.ds((at + k) * streams, size), :])
            product = times(left, jnp.concatenate(right, axis=1))
            for k in range(2):
                now = skew(product[:, k * LANES : (k + 1) * LANES])
                value = jnp.where(lower, now, before)
                before = now
                value = jnp.sum(value.reshape(small // 8, 8, LANES), axis=0)
                partial[u, pl.ds((2 * pair + k) * 8, 8), :] = value
        total = partial[u, pl.ds(0, blocks, stride=8), :]
        for j in range(1, 8):
            total = total + partial[u, pl.ds(j, blocks, stride=8), :]
        lags[pl.ds(c * blocks, blocks), :] = total * factor

    def step(i, carry):
        for u in range(ahead):
            channel(i * ahead + u, u)
        return carry

    lax.fori_loop(0, cpd // ahead, step, 0)
    flip = flip_matrix(LANES, f32)
    lags[...] = jnp.dot(lags[...], flip, preferred_element_type=f32, precision=lax.Precision.HIGHEST)
    per_part = blocks // made.shape[0]
    for k in range(blocks):
        column = pl.ds((k % per_part) * LANES, LANES)
        made[k // per_part, :, column] = lags[pl.ds(blocks - 1 - k, cpd, stride=blocks), :]


def exchange(blocks, axis):
    size = blocks.shape[0]
    me = lax.axis_index(axis)
    own = lax.dynamic_index_in_dim(blocks, me, 0, True)
    result = lax.dynamic_update_slice_in_dim(jnp.zeros_like(blocks), own, me, 0)
    for k in range(1, size):
        part = lax.dynamic_index_in_dim(blocks, (me + k) % size, 0, True)
        part = lax.ppermute(part, axis, [(i, (i + k) % size) for i in range(size)])
        result = lax.dynamic_update_slice_in_dim(result, part, (me - k) % size, 0)
    return result


def call(kernel, out_shape, scratch=(), flops=0, limit=16, specs=None):
    extra = {} if specs is None else dict(in_specs=specs[0], out_specs=specs[1])
    return pl.pallas_call(
        kernel,
        out_shape=out_shape,
        scratch_shapes=list(scratch),
        cost_estimate=pl.CostEstimate(flops=flops, bytes_accessed=1 << 20, transcendentals=0),
        compiler_params=pltpu.CompilerParams(vmem_limit_bytes=limit << 20),
        **extra,
    )


def on_device(grad_out, gate, signal, filters):
    shape = jax.ShapeDtypeStruct
    dp, seq = lax.axis_size("dp"), lax.axis_size("seq")
    tokens, channels = grad_out.shape[1:]
    segments, per, part = filters.shape
    spd = segments // dp
    cpd = spd * per
    length = tokens * seq
    halves = tokens // LANES
    blocks = length // LANES
    rows = dp * seq * cpd
    streams = 2 * dp
    size = blocks * streams
    copies = PACK // streams
    ahead = AHEAD if cpd % AHEAD == 0 else 1
    both = ("dp", "seq")
    taps = exchange(filters.reshape(dp, cpd, part // LANES, LANES), "dp")
    edge = (dp, seq, per, spd)
    anywhere = pl.BlockSpec(memory_space=pl.ANY)
    sent = call(
        functools.partial(send_kernel, edge),
        shape((dp * seq, 2 * cpd, tokens), bf16),
        (
            pltpu.VMEM((tokens, channels), bf16),
            pltpu.VMEM((tokens, channels), bf16),
            pltpu.VMEM((tokens, channels), bf16),
            pltpu.VMEM((dp * seq, 2 * cpd, tokens), bf16),
            pltpu.SemaphoreType.DMA((3, dp)),
            pltpu.SemaphoreType.DMA((dp,)),
        ),
        limit=63,
        specs=([anywhere] * 3, anywhere),
    )(grad_out[0], gate[0], signal[0])
    got = lax.all_to_all(sent, both, split_axis=0, concat_axis=0, tiled=True)
    inner = (dp, seq, cpd)
    made = call(
        functools.partial(mix_kernel, inner),
        shape((dp * seq, 2 * cpd, tokens), bf16),
        (
            pltpu.VMEM((halves, rows, LANES), f32),
            pltpu.VMEM((halves, rows, LANES), f32),
            pltpu.VMEM((ahead, PACK + size, LANES), f32),
            pltpu.VMEM((ahead, copies, 2 * size, LANES), bf16),
            pltpu.VMEM((ahead, size, LANES), f32),
            pltpu.VMEM((2, halves, rows, LANES), f32),
        ),
    )(got, taps)
    back = lax.all_to_all(made, both, split_axis=0, concat_axis=0, tiled=True)
    lags = call(
        functools.partial(tap_kernel, inner, float(dp * length) ** -0.5),
        shape((dp, cpd, part), f32),
        (
            pltpu.VMEM((halves, rows, LANES), f32),
            pltpu.VMEM((halves, rows, LANES), f32),
            pltpu.VMEM((ahead, dp, 8 + blocks, LANES), f32),
            pltpu.VMEM((ahead, PACK + size, LANES), f32),
            pltpu.VMEM((ahead, copies, 2 * size, LANES), bf16),
            pltpu.VMEM((ahead, size, LANES), f32),
            pltpu.VMEM((ahead, blocks * 8, LANES), f32),
            pltpu.VMEM((cpd * blocks, LANES), f32),
        ),
        flops=1 << 30,
    )(got)
    grad_filter = exchange(lags, "dp").reshape(segments, per, part)
    grad_signal, grad_gate = call(
        functools.partial(receive_kernel, edge),
        (shape((tokens, channels), bf16), shape((tokens, channels), bf16)),
    )(back, grad_out[0])
    return (grad_signal[None], grad_gate[None], grad_filter)


def solution(mesh):
    tokens = P("dp", "seq", None)
    taps = P(None, "seq", "dp")
    return jax.shard_map(
        on_device,
        mesh=mesh,
        in_specs=(tokens, tokens, tokens, taps),
        out_specs=(tokens, tokens, taps),
        check_vma=False,
    )
```

```python
import functools

import jax
import jax.numpy as jnp
from jax import lax
from jax.experimental import pallas as pl
from jax.experimental.pallas import tpu as pltpu
from jax.sharding import PartitionSpec as P

LANES = 128
PACK = 16
AHEAD = 2
bf16 = jnp.bfloat16
f32 = jnp.float32


def iota(shape, axis):
    return lax.broadcasted_iota(jnp.int32, shape, axis)


def flip_matrix(size, dtype):
    hit = iota((size, size), 0) + iota((size, size), 1) == size - 1
    return jnp.where(hit, 1.0, 0.0).astype(dtype)


def times(a, b):
    return jnp.dot(a, b, preferred_element_type=f32)


def gather_rows(parts):
    return parts[0] if len(parts) == 1 else jnp.concatenate(parts, axis=0)


def send_kernel(sizes, out_grad, gate, signal, sent, grads, gates, signals, made, arrived, left):
    dp, seq, per, spd = sizes
    width = per * seq * spd
    pairs = ((signal, signals), (out_grad, grads), (gate, gates))
    coming = [
        [
            pltpu.make_async_copy(
                source.at[:, pl.ds(p * width, width)],
                held.at[:, pl.ds(p * width, width)],
                arrived.at[k, p],
            )
            for k, (source, held) in enumerate(pairs)
        ]
        for p in range(dp)
    ]
    going = [
        pltpu.make_async_copy(made.at[pl.ds(p * seq, seq)], sent.at[pl.ds(p * seq, seq)], left.at[p])
        for p in range(dp)
    ]
    for copies in coming:
        for copy in copies:
            copy.start()
    for p in range(dp):
        at = pl.ds(p * width, width)
        for copy in coming[p]:
            copy.wait()
        plain = signals[:, at].astype(f32).T
        scaled = (grads[:, at].astype(f32) * gates[:, at].astype(f32)).T
        for q in range(seq):
            parts = []
            for value in (scaled, plain):
                for s in range(spd):
                    begin = (s * seq + q) * per
                    parts.append(value[begin : begin + per])
            made[p * seq + q] = gather_rows(parts).astype(bf16)
        going[p].start()
    for copy in going:
        copy.wait()


def receive_kernel(sizes, got, out_grad, grad_signal, grad_gate):
    dp, seq, per, spd = sizes
    width = per * seq
    cpd = per * spd
    for p in range(dp):
        for s in range(spd):
            begin = (p * spd + s) * width
            turned = []
            for t in range(2):
                low = t * cpd + s * per
                block = got[p * seq : (p + 1) * seq].astype(f32)
                turned.append(gather_rows([block[q, low : low + per] for q in range(seq)]).T)
            grad = out_grad[:, begin : begin + width].astype(f32)
            grad_gate[:, begin : begin + width] = (grad * turned[0]).astype(bf16)
            grad_signal[:, begin : begin + width] = turned[1].astype(bf16)


def slots(b, seq, pitch, first=1):
    return (b * (seq + 1) + first) * pitch


def clear_slots(dp, seq, pitch, held):
    for b in range(dp):
        for half in range(held.shape[0]):
            held[half, pl.ds(slots(b, seq, pitch, 0), pitch), :] = jnp.zeros((pitch, LANES), f32)


def put(held, half, at, value):
    held[half, pl.ds(at, value.shape[0]), :] = value[:, half * LANES : (half + 1) * LANES]


def stage_flipped(dp, seq, cpd, got, held):
    tokens = got.shape[2]
    flip = flip_matrix(tokens, bf16)
    for b in range(dp):
        block = got[b * seq : (b + 1) * seq, :cpd].reshape(seq * cpd, tokens)
        turned = times(block, flip)
        for q in range(seq):
            to = slots(b, seq, cpd + 1) + (seq - 1 - q) * (cpd + 1)
            for half in range(2):
                put(held, half, to, turned[q * cpd : (q + 1) * cpd])


def skew(value):
    return pltpu.roll(value, 0, 1, stride=1, stride_axis=0)


def mix_kernel(sizes, got, taps, made, plain, turned, line, shifted, result, out):
    dp, seq, cpd = sizes
    tokens = got.shape[2]
    streams = 2 * dp
    small = LANES // 2
    quarters = tokens // small
    group = quarters * streams
    size = seq * group
    pitch = cpd + 1
    ahead = line.shape[0]
    per_part = taps.shape[2]
    for b in range(dp):
        for q in range(seq):
            value = got[b * seq + q].astype(f32)[cpd:]
            for half in range(2):
                put(plain, half, slots(b, seq, pitch) + q * pitch, value)
    stage_flipped(dp, seq, cpd, got, turned)
    held = (plain, turned)
    for one in held:
        clear_slots(dp, seq, pitch, one)
    for u in range(ahead):
        shifted[u, :size] = jnp.zeros((size, LANES), bf16)
        result[u, 1, : 2 * streams + 1] = jnp.zeros((2 * streams + 1, LANES), f32)
    lower = iota((small, LANES), 1) >= iota((small, LANES), 0)
    low = iota((seq, LANES), 1) < small
    order = [(k, b, half) for k in range(2) for b in range(dp) for half in range(2)]

    def channel(c, u):
        for kind, b, half in order:
            stream = kind * dp + b
            here = held[kind][half, pl.ds(slots(b, seq, pitch) + c, seq, stride=pitch), :]
            behind = held[kind][half, pl.ds(slots(b, seq, pitch, 0) + c, seq, stride=pitch), :]
            crossed = pltpu.roll(jnp.where(low, behind, here), small, 1)
            to = 2 * half * streams + stream
            line[u, pl.ds(to, seq, stride=group + 1), :] = jnp.where(low, here, crossed)
            line[u, pl.ds(to + streams, seq, stride=group + 1), :] = jnp.where(low, crossed, behind)
        for q in range(seq):
            shifted[u, size + q * group : size + (q + 1) * group] = line[u, pl.ds(q * (group + 1), group), :].astype(bf16)
        before = jnp.zeros((small, LANES), bf16)
        sums = []
        for which in range(2):
            left, tiles = [], []
            count = size >> which
            for f in range(which * seq // 4, (which + 1) * seq // 4):
                left.append(shifted[u, pl.ds(2 * size - count - 2 * f * group, count), :])
                pieces = []
                for d in range(4 * f, 4 * f + 4):
                    row = taps[d // per_part, c, pl.ds(d % per_part, 1), :]
                    now = skew(jnp.broadcast_to(row, (small, LANES))).astype(bf16)
                    pieces.append(jnp.where(lower, now, before))
                    before = now
                tiles.append(jnp.concatenate(pieces[:2], axis=1))
                tiles.append(jnp.concatenate(pieces[2:], axis=1))
            sums.append(times(jnp.concatenate(left, axis=1), jnp.concatenate(tiles, axis=0)))
        total = jnp.concatenate([sums[0][: size // 2], sums[0][size // 2 :] + sums[1]], axis=0)
        rows = 2 * streams
        late = jnp.concatenate([jnp.zeros((rows, LANES), f32), total[: size - rows, LANES:]], axis=0)
        total = total[:, :LANES] + late
        for k in range(2 * seq):
            result[u, k % 2, pl.ds((k // 2 + 1) * (rows + 1), rows), :] = total[k * rows : (k + 1) * rows]
        for kind, b, half in order:
            stream = kind * dp + b
            first = rows + 1 + stream
            even = result[u, half, pl.ds(first, seq, stride=rows + 1), :]
            here = result[u, half, pl.ds(first + streams, seq, stride=rows + 1), :]
            at = first + streams if half else stream + streams
            behind = result[u, 1 - half, pl.ds(at, seq, stride=rows + 1), :]
            value = even + pltpu.roll(jnp.where(low, here, behind), small, 1)
            out[kind, half, pl.ds(b * seq * pitch + c, seq, stride=pitch), :] = value

    def step(i, carry):
        for u in range(ahead):
            channel(i * ahead + u, u)
        return carry

    lax.fori_loop(0, cpd // ahead, step, 0)
    flip = flip_matrix(tokens, bf16)
    for kind in (1, 0):
        for b in range(dp):
            values = []
            for q in range(seq):
                at = pl.ds((b * seq + q) * pitch, cpd)
                values.append(jnp.concatenate([out[kind, half, at, :] for half in range(2)], axis=1).astype(bf16))
            if kind == 1:
                value = times(jnp.concatenate(values, axis=0), flip).astype(bf16)
                values = [value[q * cpd : (q + 1) * cpd] for q in range(seq)]
            for q in range(seq):
                to = b * seq + (q if kind == 0 else seq - 1 - q)
                made[to, kind * cpd : (kind + 1) * cpd] = values[q]


def tap_kernel(sizes, factor, got, made, mirrored, turned, line, flat, shifted, square, partial, lags):
    dp, seq, cpd = sizes
    streams = 2 * dp
    blocks = 2 * seq
    rows = 2 * streams
    size = seq * rows
    small = LANES // 2
    pitch = cpd + 1
    ahead = line.shape[0]
    stage_flipped(dp, seq, cpd, got, turned)
    clear_slots(dp, seq, pitch, turned)
    for b in range(dp):
        for q in range(seq):
            block = got[b * seq + q].astype(f32)[cpd:]
            to = pl.ds(slots(b, seq, pitch) + (seq - 1 - q) * pitch, cpd)
            for half in range(2):
                mirrored[1 - half, to, :] = block[:, half * LANES : (half + 1) * LANES]
    for u in range(ahead):
        flat[u, :PACK] = jnp.zeros((PACK, LANES), f32)
        for k in range(PACK // streams):
            shifted[u, k, :size] = jnp.zeros((size, LANES), bf16)
    low = iota((seq, LANES), 1) < small
    lower = iota((small, LANES), 1) >= iota((small, LANES), 0)

    def channel(c, u):
        for b in range(dp):
            here = [turned[half, pl.ds(slots(b, seq, pitch) + c, seq, stride=pitch), :] for half in range(2)]
            behind = [turned[1, pl.ds(slots(b, seq, pitch, 0) + c, seq, stride=pitch), :], here[0]]
            for half in range(2):
                late = pltpu.roll(jnp.where(low, here[half], behind[half]), small, 1)
                line[u, pl.ds(half * streams + b, seq, stride=rows + 1), :] = here[half]
                line[u, pl.ds(half * streams + dp + b, seq, stride=rows + 1), :] = late
                value = mirrored[half, pl.ds(slots(b, seq, pitch) + c, seq, stride=pitch), :]
                square[u, pl.ds(half * streams + b, seq, stride=rows + 1), :] = value
                square[u, pl.ds(half * streams + dp + b, seq, stride=rows + 1), :] = pltpu.roll(value, small, 1)
        for q in range(seq):
            flat[u, PACK + q * rows : PACK + (q + 1) * rows] = line[u, pl.ds(q * (rows + 1), rows), :]
        for k in range(PACK // streams):
            shifted[u, k, size:] = flat[u, pl.ds(PACK - k * streams, size), :].astype(bf16)
        wide = jnp.concatenate([square[u, pl.ds(q * (rows + 1), rows), :] for q in range(seq)], axis=0)
        left = wide.T[:small].astype(bf16)
        before = jnp.zeros((small, LANES), f32)
        for pair in range(blocks // 2):
            right = []
            for at in (2 * pair + 1, 2 * pair + 2):
                k = -at % (PACK // streams)
                right.append(shifted[u, k, pl.ds((at + k) * streams, size), :])
            product = times(left, jnp.concatenate(right, axis=1))
            for k in range(2):
                now = skew(product[:, k * LANES : (k + 1) * LANES])
                value = jnp.where(lower, now, before)
                before = now
                value = jnp.sum(value.reshape(small // 8, 8, LANES), axis=0)
                partial[u, pl.ds((2 * pair + k) * 9, 8), :] = value
        total = partial[u, pl.ds(0, blocks, stride=9), :]
        for j in range(1, 8):
            total = total + partial[u, pl.ds(j, blocks, stride=9), :]
        lags[pl.ds(c * (blocks + 1), blocks), :] = total * factor

    def step(i, carry):
        for u in range(ahead):
            channel(i * ahead + u, u)
        return carry

    lax.fori_loop(0, cpd // ahead, step, 0)
    flip = flip_matrix(LANES, f32)
    for c in range(cpd):
        at = pl.ds(c * (blocks + 1), blocks)
        lags[at, :] = jnp.dot(lags[at, :], flip, preferred_element_type=f32, precision=lax.Precision.HIGHEST)
    per_part = blocks // made.shape[0]
    for k in range(blocks):
        column = pl.ds((k % per_part) * LANES, LANES)
        made[k // per_part, :, column] = lags[pl.ds(blocks - 1 - k, cpd, stride=blocks + 1), :]


def exchange(blocks, axis):
    size = blocks.shape[0]
    me = lax.axis_index(axis)
    own = lax.dynamic_index_in_dim(blocks, me, 0, True)
    result = lax.dynamic_update_slice_in_dim(jnp.zeros_like(blocks), own, me, 0)
    for k in range(1, size):
        part = lax.dynamic_index_in_dim(blocks, (me + k) % size, 0, True)
        part = lax.ppermute(part, axis, [(i, (i + k) % size) for i in range(size)])
        result = lax.dynamic_update_slice_in_dim(result, part, (me - k) % size, 0)
    return result


def call(kernel, out_shape, scratch=(), flops=0, limit=16, specs=None):
    extra = {} if specs is None else dict(in_specs=specs[0], out_specs=specs[1])
    return pl.pallas_call(
        kernel,
        out_shape=out_shape,
        scratch_shapes=list(scratch),
        cost_estimate=pl.CostEstimate(flops=flops, bytes_accessed=1 << 20, transcendentals=0),
        compiler_params=pltpu.CompilerParams(vmem_limit_bytes=limit << 20),
        **extra,
    )


def on_device(grad_out, gate, signal, filters):
    shape = jax.ShapeDtypeStruct
    dp, seq = lax.axis_size("dp"), lax.axis_size("seq")
    tokens, channels = grad_out.shape[1:]
    segments, per, part = filters.shape
    spd = segments // dp
    cpd = spd * per
    length = tokens * seq
    blocks = length // LANES
    streams = 2 * dp
    group = 4 * streams
    slot_rows = dp * (seq + 1) * (cpd + 1)
    line_rows = seq * (2 * streams + 1)
    ahead = AHEAD if cpd % AHEAD == 0 else 1
    both = ("dp", "seq")
    taps = exchange(filters.reshape(dp, cpd, part // LANES, LANES), "dp")
    edge = (dp, seq, per, spd)
    anywhere = pl.BlockSpec(memory_space=pl.ANY)
    sent = call(
        functools.partial(send_kernel, edge),
        shape((dp * seq, 2 * cpd, tokens), bf16),
        (
            pltpu.VMEM((tokens, channels), bf16),
            pltpu.VMEM((tokens, channels), bf16),
            pltpu.VMEM((tokens, channels), bf16),
            pltpu.VMEM((dp * seq, 2 * cpd, tokens), bf16),
            pltpu.SemaphoreType.DMA((3, dp)),
            pltpu.SemaphoreType.DMA((dp,)),
        ),
        limit=63,
        specs=([anywhere] * 3, anywhere),
    )(grad_out[0], gate[0], signal[0])
    got = lax.all_to_all(sent, both, split_axis=0, concat_axis=0, tiled=True)
    inner = (dp, seq, cpd)
    made = call(
        functools.partial(mix_kernel, inner),
        shape((dp * seq, 2 * cpd, tokens), bf16),
        (
            pltpu.VMEM((2, slot_rows, LANES), f32),
            pltpu.VMEM((2, slot_rows, LANES), f32),
            pltpu.VMEM((ahead, seq * (group + 1), LANES), f32),
            pltpu.VMEM((ahead, 2 * seq * group, LANES), bf16),
            pltpu.VMEM((ahead, 2, line_rows + 2 * streams + 1, LANES), f32),
            pltpu.VMEM((2, 2, dp * seq * (cpd + 1), LANES), f32),
        ),
    )(got, taps)
    back = lax.all_to_all(made, both, split_axis=0, concat_axis=0, tiled=True)
    lags = call(
        functools.partial(tap_kernel, inner, float(dp * length) ** -0.5),
        shape((dp, cpd, part), f32),
        (
            pltpu.VMEM((2, slot_rows, LANES), f32),
            pltpu.VMEM((2, slot_rows, LANES), f32),
            pltpu.VMEM((ahead, line_rows, LANES), f32),
            pltpu.VMEM((ahead, PACK + blocks * streams, LANES), f32),
            pltpu.VMEM((ahead, PACK // streams, 2 * blocks * streams, LANES), bf16),
            pltpu.VMEM((ahead, line_rows, LANES), f32),
            pltpu.VMEM((ahead, blocks * 9, LANES), f32),
            pltpu.VMEM((cpd * (blocks + 1), LANES), f32),
        ),
        flops=1 << 30,
    )(got)
    grad_filter = exchange(lags, "dp").reshape(segments, per, part)
    grad_signal, grad_gate = call(
        functools.partial(receive_kernel, edge),
        (shape((tokens, channels), bf16), shape((tokens, channels), bf16)),
    )(back, grad_out[0])
    return (grad_signal[None], grad_gate[None], grad_filter)


def solution(mesh):
    tokens = P("dp", "seq", None)
    taps = P(None, "seq", "dp")
    return jax.shard_map(
        on_device,
        mesh=mesh,
        in_specs=(tokens, tokens, tokens, taps),
        out_specs=(tokens, tokens, taps),
        check_vma=False,
    )
```

```python
import functools

import jax
import jax.numpy as jnp
from jax import lax
from jax.experimental import pallas as pl
from jax.experimental.pallas import tpu as pltpu
from jax.sharding import PartitionSpec as P

LANES = 128
PACK = 16
AHEAD = 2
bf16 = jnp.bfloat16
f32 = jnp.float32


def iota(shape, axis):
    return lax.broadcasted_iota(jnp.int32, shape, axis)


def flip_matrix(size, dtype):
    hit = iota((size, size), 0) + iota((size, size), 1) == size - 1
    return jnp.where(hit, 1.0, 0.0).astype(dtype)


def times(a, b):
    return jnp.dot(a, b, preferred_element_type=f32)


def gather_rows(parts):
    return parts[0] if len(parts) == 1 else jnp.concatenate(parts, axis=0)


def send_kernel(sizes, out_grad, gate, signal, sent, grads, gates, signals, made, arrived, left):
    dp, seq, per, spd = sizes
    width = per * seq * spd
    pairs = ((signal, signals), (out_grad, grads), (gate, gates))
    coming = [
        [
            pltpu.make_async_copy(
                source.at[:, pl.ds(p * width, width)],
                held.at[:, pl.ds(p * width, width)],
                arrived.at[k, p],
            )
            for k, (source, held) in enumerate(pairs)
        ]
        for p in range(dp)
    ]
    going = [
        pltpu.make_async_copy(made.at[pl.ds(p * seq, seq)], sent.at[pl.ds(p * seq, seq)], left.at[p])
        for p in range(dp)
    ]
    for copies in coming:
        for copy in copies:
            copy.start()
    flip = flip_matrix(grads.shape[0], bf16)
    for p in range(dp):
        at = pl.ds(p * width, width)
        for copy in coming[p]:
            copy.wait()
        scaled = (grads[:, at].astype(f32) * gates[:, at].astype(f32)).T
        scaled = times(scaled.astype(bf16), flip)
        plain = signals[:, at].astype(f32).T
        for q in range(seq):
            parts = []
            for value in (scaled, plain):
                for s in range(spd):
                    begin = (s * seq + q) * per
                    parts.append(value[begin : begin + per])
            made[p * seq + q] = gather_rows(parts).astype(bf16)
        going[p].start()
    for copy in going:
        copy.wait()


def receive_kernel(sizes, got, out_grad, grad_signal, grad_gate):
    dp, seq, per, spd = sizes
    width = per * seq
    cpd = per * spd
    flip = flip_matrix(got.shape[2], bf16)
    for p in range(dp):
        for s in range(spd):
            begin = (p * spd + s) * width
            turned = []
            for t in range(2):
                low = t * cpd + s * per
                block = got[p * seq : (p + 1) * seq].astype(f32)
                block = gather_rows([block[q, low : low + per] for q in range(seq)])
                turned.append((times(block.astype(bf16), flip) if t else block).T)
            grad = out_grad[:, begin : begin + width].astype(f32)
            grad_gate[:, begin : begin + width] = (grad * turned[0]).astype(bf16)
            grad_signal[:, begin : begin + width] = turned[1].astype(bf16)


def slots(b, seq, pitch, first=1):
    return (b * (seq + 1) + first) * pitch


def clear_slots(dp, seq, pitch, held):
    for b in range(dp):
        for half in range(held.shape[0]):
            held[half, pl.ds(slots(b, seq, pitch, 0), pitch), :] = jnp.zeros((pitch, LANES), f32)


def put(held, half, at, value):
    held[half, pl.ds(at, value.shape[0]), :] = value[:, half * LANES : (half + 1) * LANES]


def stage(dp, seq, cpd, got, plain, turned):
    pitch = cpd + 1
    for b in range(dp):
        for q in range(seq):
            value = got[b * seq + q].astype(f32)
            for half in range(2):
                put(plain, half, slots(b, seq, pitch) + q * pitch, value[cpd:])
                put(turned, half, slots(b, seq, pitch) + (seq - 1 - q) * pitch, value[:cpd])


def skew(value):
    return pltpu.roll(value, 0, 1, stride=1, stride_axis=0)


def mix_kernel(sizes, got, taps, made, plain, turned, line, shifted, result, out, done, left):
    dp, seq, cpd = sizes
    tokens = got.shape[2]
    streams = 2 * dp
    small = LANES // 2
    quarters = tokens // small
    group = quarters * streams
    size = seq * group
    pitch = cpd + 1
    ahead = line.shape[0]

    per_part = taps.shape[2]
    held = (plain, turned)
    stage(dp, seq, cpd, got, plain, turned)
    for one in held:
        clear_slots(dp, seq, pitch, one)
    for u in range(ahead):
        shifted[u, :size] = jnp.zeros((size, LANES), bf16)
        result[u, 1, : 2 * streams + 1] = jnp.zeros((2 * streams + 1, LANES), f32)
    lower = iota((small, LANES), 1) >= iota((small, LANES), 0)
    low = iota((seq, LANES), 1) < small
    order = [(k, b, half) for k in range(2) for b in range(dp) for half in range(2)]

    def channel(c, u):
        for kind, b, half in order:
            stream = kind * dp + b
            here = held[kind][half, pl.ds(slots(b, seq, pitch) + c, seq, stride=pitch), :]
            behind = held[kind][half, pl.ds(slots(b, seq, pitch, 0) + c, seq, stride=pitch), :]
            crossed = pltpu.roll(jnp.where(low, behind, here), small, 1)
            to = 2 * half * streams + stream
            line[u, pl.ds(to, seq, stride=group + 1), :] = jnp.where(low, here, crossed)
            line[u, pl.ds(to + streams, seq, stride=group + 1), :] = jnp.where(low, crossed, behind)
        for q in range(seq):
            shifted[u, size + q * group : size + (q + 1) * group] = line[u, pl.ds(q * (group + 1), group), :].astype(bf16)
        before = jnp.zeros((small, LANES), bf16)
        sums = []
        for which in range(2):
            blocks, tiles = [], []
            count = size >> which
            for f in range(which * seq // 4, (which + 1) * seq // 4):
                blocks.append(shifted[u, pl.ds(2 * size - count - 2 * f * group, count), :])
                pieces = []
                for d in range(4 * f, 4 * f + 4):
                    row = taps[d // per_part, c, pl.ds(d % per_part, 1), :]
                    now = skew(jnp.broadcast_to(row, (small, LANES))).astype(bf16)
                    pieces.append(jnp.where(lower, now, before))
                    before = now
                tiles.append(jnp.concatenate(pieces[:2], axis=1))
                tiles.append(jnp.concatenate(pieces[2:], axis=1))
            sums.append(times(jnp.concatenate(blocks, axis=1), jnp.concatenate(tiles, axis=0)))
        total = jnp.concatenate([sums[0][: size // 2], sums[0][size // 2 :] + sums[1]], axis=0)
        rows = 2 * streams
        late = jnp.concatenate([jnp.zeros((rows, LANES), f32), total[: size - rows, LANES:]], axis=0)
        total = total[:, :LANES] + late
        for k in range(2 * seq):
            result[u, k % 2, pl.ds((k // 2 + 1) * (rows + 1), rows), :] = total[k * rows : (k + 1) * rows]
        for kind, b, half in order:
            stream = kind * dp + b
            first = rows + 1 + stream
            even = result[u, half, pl.ds(first, seq, stride=rows + 1), :]
            here = result[u, half, pl.ds(first + streams, seq, stride=rows + 1), :]
            at = first + streams if half else stream + streams
            behind = result[u, 1 - half, pl.ds(at, seq, stride=rows + 1), :]
            value = even + pltpu.roll(jnp.where(low, here, behind), small, 1)
            out[kind, half, pl.ds(b * seq * pitch + c, seq, stride=pitch), :] = value

    parts = left.shape[0]
    each = cpd // parts
    going = []
    for part in range(parts):

        def step(i, carry):
            for u in range(ahead):
                channel(part * each + i * ahead + u, u)
            return carry

        lax.fori_loop(0, each // ahead, step, 0)
        for kind in range(2):
            to = pl.ds(kind * cpd + part * each, each)
            for b in range(dp):
                for q in range(seq):
                    at = pl.ds((b * seq + q) * pitch + part * each, each)
                    value = jnp.concatenate([out[kind, half, at, :] for half in range(2)], axis=1)
                    done[b * seq + (seq - 1 - q if kind else q), to, :] = value.astype(bf16)
            going.append(pltpu.make_async_copy(done.at[:, to, :], made.at[:, to, :], left.at[part, kind]))
            going[-1].start()
    for copy in going:
        copy.wait()


def tap_kernel(sizes, factor, got, made, mirrored, turned, line, flat, shifted, square, partial, lags):
    dp, seq, cpd = sizes
    streams = 2 * dp
    blocks = 2 * seq
    rows = 2 * streams
    size = seq * rows
    small = LANES // 2
    pitch = cpd + 1
    ahead = line.shape[0]
    clear_slots(dp, seq, pitch, turned)
    for b in range(dp):
        for q in range(seq):
            value = got[b * seq + q].astype(f32)
            to = slots(b, seq, pitch) + (seq - 1 - q) * pitch
            for half in range(2):
                put(turned, half, to, value[:cpd])
                at = pl.ds(to, cpd)
                mirrored[1 - half, at, :] = value[cpd:, half * LANES : (half + 1) * LANES]
    for u in range(ahead):
        flat[u, :PACK] = jnp.zeros((PACK, LANES), f32)
        for k in range(PACK // streams):
            shifted[u, k, :size] = jnp.zeros((size, LANES), bf16)
    low = iota((seq, LANES), 1) < small
    lower = iota((small, LANES), 1) >= iota((small, LANES), 0)

    def channel(c, u):
        for b in range(dp):
            here = [turned[half, pl.ds(slots(b, seq, pitch) + c, seq, stride=pitch), :] for half in range(2)]
            behind = [turned[1, pl.ds(slots(b, seq, pitch, 0) + c, seq, stride=pitch), :], here[0]]
            for half in range(2):
                late = pltpu.roll(jnp.where(low, here[half], behind[half]), small, 1)
                line[u, pl.ds(half * streams + b, seq, stride=rows + 1), :] = here[half]
                line[u, pl.ds(half * streams + dp + b, seq, stride=rows + 1), :] = late
                value = mirrored[half, pl.ds(slots(b, seq, pitch) + c, seq, stride=pitch), :]
                square[u, pl.ds(half * streams + b, seq, stride=rows + 1), :] = value
                square[u, pl.ds(half * streams + dp + b, seq, stride=rows + 1), :] = pltpu.roll(value, small, 1)
        for q in range(seq):
            flat[u, PACK + q * rows : PACK + (q + 1) * rows] = line[u, pl.ds(q * (rows + 1), rows), :]
        for k in range(PACK // streams):
            shifted[u, k, size:] = flat[u, pl.ds(PACK - k * streams, size), :].astype(bf16)
        wide = jnp.concatenate([square[u, pl.ds(q * (rows + 1), rows), :] for q in range(seq)], axis=0)
        left = wide.T[:small].astype(bf16)
        before = jnp.zeros((small, LANES), f32)
        for pair in range(blocks // 2):
            right = []
            for at in (2 * pair + 1, 2 * pair + 2):
                k = -at % (PACK // streams)
                right.append(shifted[u, k, pl.ds((at + k) * streams, size), :])
            product = times(left, jnp.concatenate(right, axis=1))
            for k in range(2):
                now = skew(product[:, k * LANES : (k + 1) * LANES])
                value = jnp.where(lower, now, before)
                before = now
                value = jnp.sum(value.reshape(small // 8, 8, LANES), axis=0)
                partial[u, pl.ds((2 * pair + k) * 9, 8), :] = value
        total = partial[u, pl.ds(0, blocks, stride=9), :]
        for j in range(1, 8):
            total = total + partial[u, pl.ds(j, blocks, stride=9), :]
        lags[pl.ds(c * (blocks + 1), blocks), :] = total * factor

    def step(i, carry):
        for u in range(ahead):
            channel(i * ahead + u, u)
        return carry

    lax.fori_loop(0, cpd // ahead, step, 0)
    flip = flip_matrix(LANES, f32)
    for c in range(cpd):
        at = pl.ds(c * (blocks + 1), blocks)
        lags[at, :] = jnp.dot(lags[at, :], flip, preferred_element_type=f32, precision=lax.Precision.HIGHEST)
    per_part = blocks // made.shape[0]
    for k in range(blocks):
        column = pl.ds((k % per_part) * LANES, LANES)
        made[k // per_part, :, column] = lags[pl.ds(blocks - 1 - k, cpd, stride=blocks + 1), :]


def exchange(blocks, axis):
    size = blocks.shape[0]
    me = lax.axis_index(axis)
    own = lax.dynamic_index_in_dim(blocks, me, 0, True)
    result = lax.dynamic_update_slice_in_dim(jnp.zeros_like(blocks), own, me, 0)
    for k in range(1, size):
        part = lax.dynamic_index_in_dim(blocks, (me + k) % size, 0, True)
        part = lax.ppermute(part, axis, [(i, (i + k) % size) for i in range(size)])
        result = lax.dynamic_update_slice_in_dim(result, part, (me - k) % size, 0)
    return result


def call(kernel, out_shape, scratch=(), flops=0, limit=16, specs=None):
    extra = {} if specs is None else dict(in_specs=specs[0], out_specs=specs[1])
    return pl.pallas_call(
        kernel,
        out_shape=out_shape,
        scratch_shapes=list(scratch),
        cost_estimate=pl.CostEstimate(flops=flops, bytes_accessed=1 << 20, transcendentals=0),
        compiler_params=pltpu.CompilerParams(vmem_limit_bytes=limit << 20),
        **extra,
    )


def on_device(grad_out, gate, signal, filters):
    shape = jax.ShapeDtypeStruct
    dp, seq = lax.axis_size("dp"), lax.axis_size("seq")
    tokens, channels = grad_out.shape[1:]
    segments, per, part = filters.shape
    spd = segments // dp
    cpd = spd * per
    length = tokens * seq
    blocks = length // LANES
    streams = 2 * dp
    group = 4 * streams
    slot_rows = dp * (seq + 1) * (cpd + 1)
    line_rows = seq * (2 * streams + 1)
    ahead = AHEAD if cpd % AHEAD == 0 else 1
    many = 4 if cpd % 16 == 0 else ahead
    both = ("dp", "seq")
    taps = exchange(filters.reshape(dp, cpd, part // LANES, LANES), "dp")
    edge = (dp, seq, per, spd)
    anywhere = pl.BlockSpec(memory_space=pl.ANY)
    sent = call(
        functools.partial(send_kernel, edge),
        shape((dp * seq, 2 * cpd, tokens), bf16),
        (
            pltpu.VMEM((tokens, channels), bf16),
            pltpu.VMEM((tokens, channels), bf16),
            pltpu.VMEM((tokens, channels), bf16),
            pltpu.VMEM((dp * seq, 2 * cpd, tokens), bf16),
            pltpu.SemaphoreType.DMA((3, dp)),
            pltpu.SemaphoreType.DMA((dp,)),
        ),
        limit=63,
        specs=([anywhere] * 3, anywhere),
    )(grad_out[0], gate[0], signal[0])
    got = lax.all_to_all(sent, both, split_axis=0, concat_axis=0, tiled=True)
    inner = (dp, seq, cpd)
    parts = 2 if cpd % 16 == 0 else 1
    made = call(
        functools.partial(mix_kernel, inner),
        shape((dp * seq, 2 * cpd, tokens), bf16),
        (
            pltpu.VMEM((2, slot_rows, LANES), f32),
            pltpu.VMEM((2, slot_rows, LANES), f32),
            pltpu.VMEM((many, seq * (group + 1), LANES), f32),
            pltpu.VMEM((many, 2 * seq * group, LANES), bf16),
            pltpu.VMEM((many, 2, line_rows + 2 * streams + 1, LANES), f32),
            pltpu.VMEM((2, 2, dp * seq * (cpd + 1), LANES), f32),
            pltpu.VMEM((dp * seq, 2 * cpd, tokens), bf16),
            pltpu.SemaphoreType.DMA((parts, 2)),
        ),
        specs=([pl.BlockSpec(memory_space=pltpu.VMEM)] * 2, anywhere),
    )(got, taps)
    back = lax.all_to_all(made, both, split_axis=0, concat_axis=0, tiled=True)
    lags = call(
        functools.partial(tap_kernel, inner, float(dp * length) ** -0.5),
        shape((dp, cpd, part), f32),
        (
            pltpu.VMEM((2, slot_rows, LANES), f32),
            pltpu.VMEM((2, slot_rows, LANES), f32),
            pltpu.VMEM((ahead, line_rows, LANES), f32),
            pltpu.VMEM((ahead, PACK + blocks * streams, LANES), f32),
            pltpu.VMEM((ahead, PACK // streams, 2 * blocks * streams, LANES), bf16),
            pltpu.VMEM((ahead, line_rows, LANES), f32),
            pltpu.VMEM((ahead, blocks * 9, LANES), f32),
            pltpu.VMEM((cpd * (blocks + 1), LANES), f32),
        ),
        flops=1 << 30,
    )(got)
    grad_filter = exchange(lags, "dp").reshape(segments, per, part)
    grad_signal, grad_gate = call(
        functools.partial(receive_kernel, edge),
        (shape((tokens, channels), bf16), shape((tokens, channels), bf16)),
    )(back, grad_out[0])
    return (grad_signal[None], grad_gate[None], grad_filter)


def solution(mesh):
    tokens = P("dp", "seq", None)
    taps = P(None, "seq", "dp")
    return jax.shard_map(
        on_device,
        mesh=mesh,
        in_specs=(tokens, tokens, tokens, taps),
        out_specs=(tokens, tokens, taps),
        check_vma=False,
    )
```

```python
import functools

import jax
import jax.numpy as jnp
from jax import lax
from jax.experimental import pallas as pl
from jax.experimental.pallas import tpu as pltpu
from jax.sharding import PartitionSpec as P

LANES = 128
PACK = 16
AHEAD = 2
NEAR = 2
bf16 = jnp.bfloat16
f32 = jnp.float32


def iota(shape, axis):
    return lax.broadcasted_iota(jnp.int32, shape, axis)


def flip_matrix(size, dtype):
    hit = iota((size, size), 0) + iota((size, size), 1) == size - 1
    return jnp.where(hit, 1.0, 0.0).astype(dtype)


def times(a, b):
    return jnp.dot(a, b, preferred_element_type=f32)


def gather_rows(parts):
    return parts[0] if len(parts) == 1 else jnp.concatenate(parts, axis=0)


def send_kernel(sizes, out_grad, gate, signal, sent, grads, gates, signals, made, arrived, left):
    dp, seq, per, spd = sizes
    width = per * seq * spd
    pairs = ((signal, signals), (out_grad, grads), (gate, gates))
    coming = [
        [
            pltpu.make_async_copy(
                source.at[:, pl.ds(p * width, width)],
                held.at[:, pl.ds(p * width, width)],
                arrived.at[k, p],
            )
            for k, (source, held) in enumerate(pairs)
        ]
        for p in range(dp)
    ]
    going = [
        pltpu.make_async_copy(made.at[pl.ds(p * seq, seq)], sent.at[pl.ds(p * seq, seq)], left.at[p])
        for p in range(dp)
    ]
    for copies in coming:
        for copy in copies:
            copy.start()
    flip = flip_matrix(grads.shape[0], bf16)
    for p in range(dp):
        at = pl.ds(p * width, width)
        for copy in coming[p]:
            copy.wait()
        scaled = (grads[:, at].astype(f32) * gates[:, at].astype(f32)).T
        scaled = times(scaled.astype(bf16), flip)
        plain = signals[:, at].astype(f32).T
        for q in range(seq):
            parts = []
            for value in (scaled, plain):
                for s in range(spd):
                    begin = (s * seq + q) * per
                    parts.append(value[begin : begin + per])
            made[p * seq + q] = gather_rows(parts).astype(bf16)
        going[p].start()
    for copy in going:
        copy.wait()


def receive_kernel(sizes, got, out_grad, grad_signal, grad_gate):
    dp, seq, per, spd = sizes
    width = per * seq
    cpd = per * spd
    flip = flip_matrix(got.shape[2], bf16)
    for p in range(dp):
        for s in range(spd):
            begin = (p * spd + s) * width
            turned = []
            for t in range(2):
                low = t * cpd + s * per
                block = got[p * seq : (p + 1) * seq].astype(f32)
                block = gather_rows([block[q, low : low + per] for q in range(seq)])
                turned.append((times(block.astype(bf16), flip) if t else block).T)
            grad = out_grad[:, begin : begin + width].astype(f32)
            grad_gate[:, begin : begin + width] = (grad * turned[0]).astype(bf16)
            grad_signal[:, begin : begin + width] = turned[1].astype(bf16)


def slots(b, seq, pitch, first=1):
    return (b * (seq + 1) + first) * pitch


def clear_slots(dp, seq, pitch, held):
    for b in range(dp):
        for half in range(held.shape[0]):
            held[half, pl.ds(slots(b, seq, pitch, 0), pitch), :] = jnp.zeros((pitch, LANES), f32)


def put(held, half, at, value):
    held[half, pl.ds(at, value.shape[0]), :] = value[:, half * LANES : (half + 1) * LANES]


def stage(dp, seq, cpd, got, plain, turned):
    pitch = cpd + 1
    for b in range(dp):
        for q in range(seq):
            value = got[b * seq + q].astype(f32)
            for half in range(2):
                put(plain, half, slots(b, seq, pitch) + q * pitch, value[cpd:])
                put(turned, half, slots(b, seq, pitch) + (seq - 1 - q) * pitch, value[:cpd])


def skew(value):
    return pltpu.roll(value, 0, 1, stride=1, stride_axis=0)


def mix_kernel(sizes, got, taps, made, plain, turned, line, shifted, windows, result, out, done, left):
    dp, seq, cpd = sizes
    tokens = got.shape[2]
    streams = 2 * dp
    small = LANES // 2
    quarters = tokens // small
    group = quarters * streams
    size = seq * group
    pitch = cpd + 1
    ahead = line.shape[0]

    per_part = taps.shape[2]
    held = (plain, turned)
    stage(dp, seq, cpd, got, plain, turned)
    for one in held:
        clear_slots(dp, seq, pitch, one)
    for u in range(ahead):
        shifted[u, :size] = jnp.zeros((size, LANES), bf16)
        result[u, 1, : 2 * streams + 1] = jnp.zeros((2 * streams + 1, LANES), f32)
    lower = iota((small, LANES), 1) >= iota((small, LANES), 0)
    low = iota((seq, LANES), 1) < small
    order = [(k, b, half) for k in range(2) for b in range(dp) for half in range(2)]

    def build(c, u):
        for kind, b, half in order:
            stream = kind * dp + b
            here = held[kind][half, pl.ds(slots(b, seq, pitch) + c, seq, stride=pitch), :]
            behind = held[kind][half, pl.ds(slots(b, seq, pitch, 0) + c, seq, stride=pitch), :]
            crossed = pltpu.roll(jnp.where(low, behind, here), small, 1)
            to = 2 * half * streams + stream
            line[u, pl.ds(to, seq, stride=group + 1), :] = jnp.where(low, here, crossed)
            line[u, pl.ds(to + streams, seq, stride=group + 1), :] = jnp.where(low, crossed, behind)
        for q in range(seq):
            shifted[u, size + q * group : size + (q + 1) * group] = line[u, pl.ds(q * (group + 1), group), :].astype(bf16)
        before = jnp.zeros((small, LANES), bf16)
        for d in range(2 * seq):
            row = taps[d // per_part, c, pl.ds(d % per_part, 1), :]
            now = skew(jnp.broadcast_to(row, (small, LANES))).astype(bf16)
            windows[u, d % 2, pl.ds((d // 2) * small, small), :] = jnp.where(lower, now, before)
            before = now

    def apply(c, u):
        deep = seq * small // 2
        sums = []
        for which in range(2):
            blocks = []
            count = size >> which
            for f in range(which * seq // 4, (which + 1) * seq // 4):
                blocks.append(shifted[u, pl.ds(2 * size - count - 2 * f * group, count), :])
            tiles = [windows[u, k, pl.ds(which * deep, deep), :] for k in range(2)]
            sums.append(times(jnp.concatenate(blocks, axis=1), jnp.concatenate(tiles, axis=1)))
        total = jnp.concatenate([sums[0][: size // 2], sums[0][size // 2 :] + sums[1]], axis=0)
        rows = 2 * streams
        late = jnp.concatenate([jnp.zeros((rows, LANES), f32), total[: size - rows, LANES:]], axis=0)
        total = total[:, :LANES] + late
        for k in range(2 * seq):
            result[u, k % 2, pl.ds((k // 2 + 1) * (rows + 1), rows), :] = total[k * rows : (k + 1) * rows]
        for kind, b, half in order:
            stream = kind * dp + b
            first = rows + 1 + stream
            even = result[u, half, pl.ds(first, seq, stride=rows + 1), :]
            here = result[u, half, pl.ds(first + streams, seq, stride=rows + 1), :]
            at = first + streams if half else stream + streams
            behind = result[u, 1 - half, pl.ds(at, seq, stride=rows + 1), :]
            value = even + pltpu.roll(jnp.where(low, here, behind), small, 1)
            out[kind, half, pl.ds(b * seq * pitch + c, seq, stride=pitch), :] = value

    parts = left.shape[0]
    each = cpd // parts

    def going(part, kind):
        to = pl.ds(kind * cpd + part * each, each)
        return pltpu.make_async_copy(done.at[:, to, :], made.at[:, to, :], left.at[part, kind])

    def finish(part):
        for kind in range(2):
            to = pl.ds(kind * cpd + part * each, each)
            for b in range(dp):
                for q in range(seq):
                    at = pl.ds((b * seq + q) * pitch + part * each, each)
                    value = jnp.concatenate([out[kind, half, at, :] for half in range(2)], axis=1)
                    done[b * seq + (seq - 1 - q if kind else q), to, :] = value.astype(bf16)
            going(part, kind).start()

    near = ahead // 2
    pairs = cpd // ahead

    def each_of(work, first, side):
        for u in range(near):
            work(first + u, side * near + u)

    def step(k, carry):
        if parts > 1:
            pl.when(k == pairs // parts)(lambda: finish(0))
        each_of(build, k * ahead + near, 1)
        each_of(apply, k * ahead, 0)
        each_of(build, k * ahead + ahead, 0)
        each_of(apply, k * ahead + near, 1)
        return carry

    each_of(build, 0, 0)
    lax.fori_loop(0, pairs - 1, step, 0)
    each_of(build, cpd - near, 1)
    each_of(apply, cpd - ahead, 0)
    each_of(apply, cpd - near, 1)
    finish(parts - 1)
    for part in range(parts):
        for kind in range(2):
            going(part, kind).wait()


def tap_kernel(sizes, factor, got, made, mirrored, turned, line, flat, shifted, square, partial, lags):
    dp, seq, cpd = sizes
    streams = 2 * dp
    blocks = 2 * seq
    rows = 2 * streams
    size = seq * rows
    small = LANES // 2
    pitch = cpd + 1
    ahead = line.shape[0]
    clear_slots(dp, seq, pitch, turned)
    for b in range(dp):
        for q in range(seq):
            value = got[b * seq + q].astype(f32)
            to = slots(b, seq, pitch) + (seq - 1 - q) * pitch
            for half in range(2):
                put(turned, half, to, value[:cpd])
                at = pl.ds(to, cpd)
                mirrored[1 - half, at, :] = value[cpd:, half * LANES : (half + 1) * LANES]
    for u in range(ahead):
        flat[u, :PACK] = jnp.zeros((PACK, LANES), f32)
        for k in range(PACK // streams):
            shifted[u, k, :size] = jnp.zeros((size, LANES), bf16)
    low = iota((seq, LANES), 1) < small
    lower = iota((small, LANES), 1) >= iota((small, LANES), 0)

    def channel(c, u):
        for b in range(dp):
            here = [turned[half, pl.ds(slots(b, seq, pitch) + c, seq, stride=pitch), :] for half in range(2)]
            behind = [turned[1, pl.ds(slots(b, seq, pitch, 0) + c, seq, stride=pitch), :], here[0]]
            for half in range(2):
                late = pltpu.roll(jnp.where(low, here[half], behind[half]), small, 1)
                line[u, pl.ds(half * streams + b, seq, stride=rows + 1), :] = here[half]
                line[u, pl.ds(half * streams + dp + b, seq, stride=rows + 1), :] = late
                value = mirrored[half, pl.ds(slots(b, seq, pitch) + c, seq, stride=pitch), :]
                square[u, pl.ds(half * streams + b, seq, stride=rows + 1), :] = value
                square[u, pl.ds(half * streams + dp + b, seq, stride=rows + 1), :] = pltpu.roll(value, small, 1)
        for q in range(seq):
            flat[u, PACK + q * rows : PACK + (q + 1) * rows] = line[u, pl.ds(q * (rows + 1), rows), :]
        for k in range(PACK // streams):
            shifted[u, k, size:] = flat[u, pl.ds(PACK - k * streams, size), :].astype(bf16)
        wide = jnp.concatenate([square[u, pl.ds(q * (rows + 1), rows), :] for q in range(seq)], axis=0)
        left = wide.T[:small].astype(bf16)
        before = jnp.zeros((small, LANES), f32)
        for pair in range(blocks // 2):
            right = []
            for at in (2 * pair + 1, 2 * pair + 2):
                k = -at % (PACK // streams)
                right.append(shifted[u, k, pl.ds((at + k) * streams, size), :])
            product = times(left, jnp.concatenate(right, axis=1))
            for k in range(2):
                now = skew(product[:, k * LANES : (k + 1) * LANES])
                value = jnp.where(lower, now, before)
                before = now
                value = jnp.sum(value.reshape(small // 8, 8, LANES), axis=0)
                partial[u, pl.ds((2 * pair + k) * 9, 8), :] = value
        total = partial[u, pl.ds(0, blocks, stride=9), :]
        for j in range(1, 8):
            total = total + partial[u, pl.ds(j, blocks, stride=9), :]
        lags[pl.ds(c * (blocks + 1), blocks), :] = total * factor

    def step(i, carry):
        for u in range(ahead):
            channel(i * ahead + u, u)
        return carry

    lax.fori_loop(0, cpd // ahead, step, 0)
    flip = flip_matrix(LANES, f32)
    for c in range(cpd):
        at = pl.ds(c * (blocks + 1), blocks)
        lags[at, :] = jnp.dot(lags[at, :], flip, preferred_element_type=f32, precision=lax.Precision.HIGHEST)
    per_part = blocks // made.shape[0]
    for k in range(blocks):
        column = pl.ds((k % per_part) * LANES, LANES)
        made[k // per_part, :, column] = lags[pl.ds(blocks - 1 - k, cpd, stride=blocks + 1), :]


def exchange(blocks, axis):
    size = blocks.shape[0]
    me = lax.axis_index(axis)
    own = lax.dynamic_index_in_dim(blocks, me, 0, True)
    result = lax.dynamic_update_slice_in_dim(jnp.zeros_like(blocks), own, me, 0)
    for k in range(1, size):
        part = lax.dynamic_index_in_dim(blocks, (me + k) % size, 0, True)
        part = lax.ppermute(part, axis, [(i, (i + k) % size) for i in range(size)])
        result = lax.dynamic_update_slice_in_dim(result, part, (me - k) % size, 0)
    return result


def call(kernel, out_shape, scratch=(), flops=0, limit=24, specs=None):
    extra = {} if specs is None else dict(in_specs=specs[0], out_specs=specs[1])
    return pl.pallas_call(
        kernel,
        out_shape=out_shape,
        scratch_shapes=list(scratch),
        cost_estimate=pl.CostEstimate(flops=flops, bytes_accessed=1 << 20, transcendentals=0),
        compiler_params=pltpu.CompilerParams(vmem_limit_bytes=limit << 20),
        **extra,
    )


def on_device(grad_out, gate, signal, filters):
    shape = jax.ShapeDtypeStruct
    dp, seq = lax.axis_size("dp"), lax.axis_size("seq")
    tokens, channels = grad_out.shape[1:]
    segments, per, part = filters.shape
    spd = segments // dp
    cpd = spd * per
    length = tokens * seq
    blocks = length // LANES
    streams = 2 * dp
    group = 4 * streams
    slot_rows = dp * (seq + 1) * (cpd + 1)
    line_rows = seq * (2 * streams + 1)
    ahead = AHEAD if cpd % AHEAD == 0 else 1
    many = 2 * NEAR if cpd % (2 * NEAR) == 0 else 2
    both = ("dp", "seq")
    taps = exchange(filters.reshape(dp, cpd, part // LANES, LANES), "dp")
    edge = (dp, seq, per, spd)
    anywhere = pl.BlockSpec(memory_space=pl.ANY)
    sent = call(
        functools.partial(send_kernel, edge),
        shape((dp * seq, 2 * cpd, tokens), bf16),
        (
            pltpu.VMEM((tokens, channels), bf16),
            pltpu.VMEM((tokens, channels), bf16),
            pltpu.VMEM((tokens, channels), bf16),
            pltpu.VMEM((dp * seq, 2 * cpd, tokens), bf16),
            pltpu.SemaphoreType.DMA((3, dp)),
            pltpu.SemaphoreType.DMA((dp,)),
        ),
        limit=63,
        specs=([anywhere] * 3, anywhere),
    )(grad_out[0], gate[0], signal[0])
    got = lax.all_to_all(sent, both, split_axis=0, concat_axis=0, tiled=True)
    inner = (dp, seq, cpd)
    parts = 2 if cpd % (4 * many) == 0 else 1
    made = call(
        functools.partial(mix_kernel, inner),
        shape((dp * seq, 2 * cpd, tokens), bf16),
        (
            pltpu.VMEM((2, slot_rows, LANES), f32),
            pltpu.VMEM((2, slot_rows, LANES), f32),
            pltpu.VMEM((many, seq * (group + 1), LANES), f32),
            pltpu.VMEM((many, 2 * seq * group, LANES), bf16),
            pltpu.VMEM((many, 2, seq * LANES // 2, LANES), bf16),
            pltpu.VMEM((many, 2, line_rows + 2 * streams + 1, LANES), f32),
            pltpu.VMEM((2, 2, dp * seq * (cpd + 1), LANES), f32),
            pltpu.VMEM((dp * seq, 2 * cpd, tokens), bf16),
            pltpu.SemaphoreType.DMA((parts, 2)),
        ),
        specs=([pl.BlockSpec(memory_space=pltpu.VMEM)] * 2, anywhere),
    )(got, taps)
    back = lax.all_to_all(made, both, split_axis=0, concat_axis=0, tiled=True)
    lags = call(
        functools.partial(tap_kernel, inner, float(dp * length) ** -0.5),
        shape((dp, cpd, part), f32),
        (
            pltpu.VMEM((2, slot_rows, LANES), f32),
            pltpu.VMEM((2, slot_rows, LANES), f32),
            pltpu.VMEM((ahead, line_rows, LANES), f32),
            pltpu.VMEM((ahead, PACK + blocks * streams, LANES), f32),
            pltpu.VMEM((ahead, PACK // streams, 2 * blocks * streams, LANES), bf16),
            pltpu.VMEM((ahead, line_rows, LANES), f32),
            pltpu.VMEM((ahead, blocks * 9, LANES), f32),
            pltpu.VMEM((cpd * (blocks + 1), LANES), f32),
        ),
        flops=1 << 30,
    )(got)
    grad_filter = exchange(lags, "dp").reshape(segments, per, part)
    grad_signal, grad_gate = call(
        functools.partial(receive_kernel, edge),
        (shape((tokens, channels), bf16), shape((tokens, channels), bf16)),
    )(back, grad_out[0])
    return (grad_signal[None], grad_gate[None], grad_filter)


def solution(mesh):
    tokens = P("dp", "seq", None)
    taps = P(None, "seq", "dp")
    return jax.shard_map(
        on_device,
        mesh=mesh,
        in_specs=(tokens, tokens, tokens, taps),
        out_specs=(tokens, tokens, taps),
        check_vma=False,
    )
```

```python
import functools

import jax
import jax.numpy as jnp
from jax import lax
from jax.experimental import pallas as pl
from jax.experimental.pallas import tpu as pltpu
from jax.sharding import PartitionSpec as P

LANES = 128
PACK = 16
AHEAD = 2
NEAR = 2
bf16 = jnp.bfloat16
f32 = jnp.float32


def iota(shape, axis):
    return lax.broadcasted_iota(jnp.int32, shape, axis)


def flip_matrix(size, dtype):
    hit = iota((size, size), 0) + iota((size, size), 1) == size - 1
    return jnp.where(hit, 1.0, 0.0).astype(dtype)


def times(a, b):
    return jnp.dot(a, b, preferred_element_type=f32)


def gather_rows(parts):
    return parts[0] if len(parts) == 1 else jnp.concatenate(parts, axis=0)


def send_kernel(sizes, out_grad, gate, signal, sent, grads, gates, signals, made, arrived, left):
    dp, seq, per, spd = sizes
    width = per * seq * spd
    pairs = ((signal, signals), (out_grad, grads), (gate, gates))
    coming = [
        [
            pltpu.make_async_copy(
                source.at[:, pl.ds(p * width, width)],
                held.at[:, pl.ds(p * width, width)],
                arrived.at[k, p],
            )
            for k, (source, held) in enumerate(pairs)
        ]
        for p in range(dp)
    ]
    going = [
        pltpu.make_async_copy(made.at[pl.ds(p * seq, seq)], sent.at[pl.ds(p * seq, seq)], left.at[p])
        for p in range(dp)
    ]
    for copies in coming:
        for copy in copies:
            copy.start()
    flip = flip_matrix(grads.shape[0], bf16)
    for p in range(dp):
        at = pl.ds(p * width, width)
        for copy in coming[p]:
            copy.wait()
        scaled = (grads[:, at].astype(f32) * gates[:, at].astype(f32)).T
        scaled = times(scaled.astype(bf16), flip)
        plain = signals[:, at].astype(f32).T
        for q in range(seq):
            parts = []
            for value in (scaled, plain):
                for s in range(spd):
                    begin = (s * seq + q) * per
                    parts.append(value[begin : begin + per])
            made[p * seq + q] = gather_rows(parts).astype(bf16)
        going[p].start()
    for copy in going:
        copy.wait()


def receive_kernel(sizes, got, out_grad, grad_signal, grad_gate):
    dp, seq, per, spd = sizes
    width = per * seq
    cpd = per * spd
    flip = flip_matrix(got.shape[2], bf16)
    for p in range(dp):
        for s in range(spd):
            begin = (p * spd + s) * width
            turned = []
            for t in range(2):
                low = t * cpd + s * per
                block = got[p * seq : (p + 1) * seq].astype(f32)
                block = gather_rows([block[q, low : low + per] for q in range(seq)])
                turned.append((times(block.astype(bf16), flip) if t else block).T)
            grad = out_grad[:, begin : begin + width].astype(f32)
            grad_gate[:, begin : begin + width] = (grad * turned[0]).astype(bf16)
            grad_signal[:, begin : begin + width] = turned[1].astype(bf16)


def slots(b, seq, pitch, first=1):
    return (b * (seq + 1) + first) * pitch


def clear_slots(dp, seq, pitch, held):
    for b in range(dp):
        for half in range(held.shape[0]):
            held[half, pl.ds(slots(b, seq, pitch, 0), pitch), :] = jnp.zeros((pitch, LANES), f32)


def put(held, half, at, value):
    held[half, pl.ds(at, value.shape[0]), :] = value[:, half * LANES : (half + 1) * LANES]


def stage(dp, seq, cpd, got, plain, turned):
    pitch = cpd + 1
    for b in range(dp):
        for q in range(seq):
            value = got[b * seq + q].astype(f32)
            for half in range(2):
                put(plain, half, slots(b, seq, pitch) + q * pitch, value[cpd:])
                put(turned, half, slots(b, seq, pitch) + (seq - 1 - q) * pitch, value[:cpd])


def skew(value):
    return pltpu.roll(value, 0, 1, stride=1, stride_axis=0)


def filter_windows(taps, c, seq, lower, store):
    per_part = taps.shape[2]
    small = LANES // 2
    before = jnp.zeros((small, LANES), bf16)
    for d in range(2 * seq):
        row = taps[d // per_part, c, pl.ds(d % per_part, 1), :]
        now = skew(jnp.broadcast_to(row, (small, LANES))).astype(bf16)
        store(d % 2, pl.ds((d // 2) * small, small), jnp.where(lower, now, before))
        before = now


def window_kernel(seq, taps, made):
    small = LANES // 2
    lower = iota((small, LANES), 1) >= iota((small, LANES), 0)

    def channel(c, carry):
        def store(k, rows, value):
            made[c, k, rows, :] = value

        filter_windows(taps, c, seq, lower, store)
        return carry

    lax.fori_loop(0, made.shape[0], channel, 0)


def mix_kernel(sizes, got, taps, ready, made, plain, turned, line, shifted, windows, result, out, done, left):
    dp, seq, cpd = sizes
    tokens = got.shape[2]
    streams = 2 * dp
    small = LANES // 2
    quarters = tokens // small
    group = quarters * streams
    size = seq * group
    pitch = cpd + 1
    ahead = line.shape[0]

    held = (plain, turned)
    stage(dp, seq, cpd, got, plain, turned)
    for one in held:
        clear_slots(dp, seq, pitch, one)
    for u in range(ahead):
        shifted[u, :size] = jnp.zeros((size, LANES), bf16)
        result[u, 1, : 2 * streams + 1] = jnp.zeros((2 * streams + 1, LANES), f32)
    lower = iota((small, LANES), 1) >= iota((small, LANES), 0)
    low = iota((seq, LANES), 1) < small
    order = [(k, b, half) for k in range(2) for b in range(dp) for half in range(2)]

    def build(c, u, early=False):
        for kind, b, half in order:
            stream = kind * dp + b
            here = held[kind][half, pl.ds(slots(b, seq, pitch) + c, seq, stride=pitch), :]
            behind = held[kind][half, pl.ds(slots(b, seq, pitch, 0) + c, seq, stride=pitch), :]
            crossed = pltpu.roll(jnp.where(low, behind, here), small, 1)
            to = 2 * half * streams + stream
            line[u, pl.ds(to, seq, stride=group + 1), :] = jnp.where(low, here, crossed)
            line[u, pl.ds(to + streams, seq, stride=group + 1), :] = jnp.where(low, crossed, behind)
        for q in range(seq):
            shifted[u, size + q * group : size + (q + 1) * group] = line[u, pl.ds(q * (group + 1), group), :].astype(bf16)
        if not early:

            def store(k, rows, value):
                windows[u, k, rows, :] = value

            filter_windows(taps, c, seq, lower, store)

    def apply(c, u, early=False):
        deep = seq * small // 2
        sums = []
        for which in range(2):
            blocks = []
            count = size >> which
            for f in range(which * seq // 4, (which + 1) * seq // 4):
                blocks.append(shifted[u, pl.ds(2 * size - count - 2 * f * group, count), :])
            source, at = (ready, c) if early else (windows, u)
            tiles = [source[at, k, pl.ds(which * deep, deep), :] for k in range(2)]
            sums.append(times(jnp.concatenate(blocks, axis=1), jnp.concatenate(tiles, axis=1)))
        total = jnp.concatenate([sums[0][: size // 2], sums[0][size // 2 :] + sums[1]], axis=0)
        rows = 2 * streams
        late = jnp.concatenate([jnp.zeros((rows, LANES), f32), total[: size - rows, LANES:]], axis=0)
        total = total[:, :LANES] + late
        for k in range(2 * seq):
            result[u, k % 2, pl.ds((k // 2 + 1) * (rows + 1), rows), :] = total[k * rows : (k + 1) * rows]
        for kind, b, half in order:
            stream = kind * dp + b
            first = rows + 1 + stream
            even = result[u, half, pl.ds(first, seq, stride=rows + 1), :]
            here = result[u, half, pl.ds(first + streams, seq, stride=rows + 1), :]
            at = first + streams if half else stream + streams
            behind = result[u, 1 - half, pl.ds(at, seq, stride=rows + 1), :]
            value = even + pltpu.roll(jnp.where(low, here, behind), small, 1)
            out[kind, half, pl.ds(b * seq * pitch + c, seq, stride=pitch), :] = value

    parts = left.shape[0]
    each = cpd // parts

    def going(part, kind):
        to = pl.ds(kind * cpd + part * each, each)
        return pltpu.make_async_copy(done.at[:, to, :], made.at[:, to, :], left.at[part, kind])

    def finish(part):
        for kind in range(2):
            to = pl.ds(kind * cpd + part * each, each)
            for b in range(dp):
                for q in range(seq):
                    at = pl.ds((b * seq + q) * pitch + part * each, each)
                    value = jnp.concatenate([out[kind, half, at, :] for half in range(2)], axis=1)
                    done[b * seq + (seq - 1 - q if kind else q), to, :] = value.astype(bf16)
            going(part, kind).start()

    near = ahead // 2
    pairs = cpd // ahead

    def each_of(work, first, side, early=False):
        for u in range(near):
            work(first + u, side * near + u, early)

    def step(k, carry):
        if parts > 1:
            pl.when(k == pairs // parts)(lambda: finish(0))
        each_of(build, k * ahead + near, 1)
        each_of(apply, k * ahead, 0)
        each_of(build, k * ahead + ahead, 0)
        each_of(apply, k * ahead + near, 1)
        return carry

    begin = ready.shape[0] // ahead
    each_of(build, 0, 0, begin > 0)
    if begin:
        each_of(build, near, 1, True)
        each_of(apply, 0, 0, True)
        each_of(build, ahead, 0)
        each_of(apply, near, 1, True)
    lax.fori_loop(begin, pairs - 1, step, 0)
    each_of(build, cpd - near, 1)
    each_of(apply, cpd - ahead, 0)
    each_of(apply, cpd - near, 1)
    finish(parts - 1)
    for part in range(parts):
        for kind in range(2):
            going(part, kind).wait()


def tap_kernel(sizes, factor, got, made, mirrored, turned, line, flat, shifted, square, partial, lags):
    dp, seq, cpd = sizes
    streams = 2 * dp
    blocks = 2 * seq
    rows = 2 * streams
    size = seq * rows
    small = LANES // 2
    pitch = cpd + 1
    ahead = line.shape[0]
    clear_slots(dp, seq, pitch, turned)
    for b in range(dp):
        for q in range(seq):
            value = got[b * seq + q].astype(f32)
            to = slots(b, seq, pitch) + (seq - 1 - q) * pitch
            for half in range(2):
                put(turned, half, to, value[:cpd])
                at = pl.ds(to, cpd)
                mirrored[1 - half, at, :] = value[cpd:, half * LANES : (half + 1) * LANES]
    for u in range(ahead):
        flat[u, :PACK] = jnp.zeros((PACK, LANES), f32)
        for k in range(PACK // streams):
            shifted[u, k, :size] = jnp.zeros((size, LANES), bf16)
    low = iota((seq, LANES), 1) < small
    lower = iota((small, LANES), 1) >= iota((small, LANES), 0)

    def channel(c, u):
        for b in range(dp):
            here = [turned[half, pl.ds(slots(b, seq, pitch) + c, seq, stride=pitch), :] for half in range(2)]
            behind = [turned[1, pl.ds(slots(b, seq, pitch, 0) + c, seq, stride=pitch), :], here[0]]
            for half in range(2):
                late = pltpu.roll(jnp.where(low, here[half], behind[half]), small, 1)
                line[u, pl.ds(half * streams + b, seq, stride=rows + 1), :] = here[half]
                line[u, pl.ds(half * streams + dp + b, seq, stride=rows + 1), :] = late
                value = mirrored[half, pl.ds(slots(b, seq, pitch) + c, seq, stride=pitch), :]
                square[u, pl.ds(half * streams + b, seq, stride=rows + 1), :] = value
                square[u, pl.ds(half * streams + dp + b, seq, stride=rows + 1), :] = pltpu.roll(value, small, 1)
        for q in range(seq):
            flat[u, PACK + q * rows : PACK + (q + 1) * rows] = line[u, pl.ds(q * (rows + 1), rows), :]
        for k in range(PACK // streams):
            shifted[u, k, size:] = flat[u, pl.ds(PACK - k * streams, size), :].astype(bf16)
        wide = jnp.concatenate([square[u, pl.ds(q * (rows + 1), rows), :] for q in range(seq)], axis=0)
        left = wide.T[:small].astype(bf16)
        before = jnp.zeros((small, LANES), f32)
        for pair in range(blocks // 2):
            right = []
            for at in (2 * pair + 1, 2 * pair + 2):
                k = -at % (PACK // streams)
                right.append(shifted[u, k, pl.ds((at + k) * streams, size), :])
            product = times(left, jnp.concatenate(right, axis=1))
            for k in range(2):
                now = skew(product[:, k * LANES : (k + 1) * LANES])
                value = jnp.where(lower, now, before)
                before = now
                value = jnp.sum(value.reshape(small // 8, 8, LANES), axis=0)
                partial[u, pl.ds((2 * pair + k) * 9, 8), :] = value
        total = partial[u, pl.ds(0, blocks, stride=9), :]
        for j in range(1, 8):
            total = total + partial[u, pl.ds(j, blocks, stride=9), :]
        lags[pl.ds(c * (blocks + 1), blocks), :] = total * factor

    def step(i, carry):
        for u in range(ahead):
            channel(i * ahead + u, u)
        return carry

    lax.fori_loop(0, cpd // ahead, step, 0)
    flip = flip_matrix(LANES, f32)
    for c in range(cpd):
        at = pl.ds(c * (blocks + 1), blocks)
        lags[at, :] = jnp.dot(lags[at, :], flip, preferred_element_type=f32, precision=lax.Precision.HIGHEST)
    per_part = blocks // made.shape[0]
    for k in range(blocks):
        column = pl.ds((k % per_part) * LANES, LANES)
        made[k // per_part, :, column] = lags[pl.ds(blocks - 1 - k, cpd, stride=blocks + 1), :]


def exchange(blocks, axis):
    size = blocks.shape[0]
    me = lax.axis_index(axis)
    own = lax.dynamic_index_in_dim(blocks, me, 0, True)
    result = lax.dynamic_update_slice_in_dim(jnp.zeros_like(blocks), own, me, 0)
    for k in range(1, size):
        part = lax.dynamic_index_in_dim(blocks, (me + k) % size, 0, True)
        part = lax.ppermute(part, axis, [(i, (i + k) % size) for i in range(size)])
        result = lax.dynamic_update_slice_in_dim(result, part, (me - k) % size, 0)
    return result


def call(kernel, out_shape, scratch=(), flops=0, limit=24, specs=None):
    extra = {} if specs is None else dict(in_specs=specs[0], out_specs=specs[1])
    return pl.pallas_call(
        kernel,
        out_shape=out_shape,
        scratch_shapes=list(scratch),
        cost_estimate=pl.CostEstimate(flops=flops, bytes_accessed=1 << 20, transcendentals=0),
        compiler_params=pltpu.CompilerParams(vmem_limit_bytes=limit << 20),
        **extra,
    )


def on_device(grad_out, gate, signal, filters):
    shape = jax.ShapeDtypeStruct
    dp, seq = lax.axis_size("dp"), lax.axis_size("seq")
    tokens, channels = grad_out.shape[1:]
    segments, per, part = filters.shape
    spd = segments // dp
    cpd = spd * per
    length = tokens * seq
    blocks = length // LANES
    streams = 2 * dp
    group = 4 * streams
    slot_rows = dp * (seq + 1) * (cpd + 1)
    line_rows = seq * (2 * streams + 1)
    ahead = AHEAD if cpd % AHEAD == 0 else 1
    many = 2 * NEAR if cpd % (2 * NEAR) == 0 else 2
    both = ("dp", "seq")
    taps = exchange(filters.reshape(dp, cpd, part // LANES, LANES), "dp")
    edge = (dp, seq, per, spd)
    anywhere = pl.BlockSpec(memory_space=pl.ANY)
    sent = call(
        functools.partial(send_kernel, edge),
        shape((dp * seq, 2 * cpd, tokens), bf16),
        (
            pltpu.VMEM((tokens, channels), bf16),
            pltpu.VMEM((tokens, channels), bf16),
            pltpu.VMEM((tokens, channels), bf16),
            pltpu.VMEM((dp * seq, 2 * cpd, tokens), bf16),
            pltpu.SemaphoreType.DMA((3, dp)),
            pltpu.SemaphoreType.DMA((dp,)),
        ),
        limit=63,
        specs=([anywhere] * 3, anywhere),
    )(grad_out[0], gate[0], signal[0])
    got = lax.all_to_all(sent, both, split_axis=0, concat_axis=0, tiled=True)
    inner = (dp, seq, cpd)
    pairs = cpd // many
    ready = call(
        functools.partial(window_kernel, seq),
        shape((many if pairs > 2 else 1, 2, seq * LANES // 2, LANES), bf16),
        flops=1 << 30,
        specs=([pl.BlockSpec(memory_space=pltpu.VMEM)], pl.BlockSpec(memory_space=pltpu.VMEM)),
    )(taps)
    parts = 2 if cpd % (4 * many) == 0 else 1
    made = call(
        functools.partial(mix_kernel, inner),
        shape((dp * seq, 2 * cpd, tokens), bf16),
        (
            pltpu.VMEM((2, slot_rows, LANES), f32),
            pltpu.VMEM((2, slot_rows, LANES), f32),
            pltpu.VMEM((many, seq * (group + 1), LANES), f32),
            pltpu.VMEM((many, 2 * seq * group, LANES), bf16),
            pltpu.VMEM((many, 2, seq * LANES // 2, LANES), bf16),
            pltpu.VMEM((many, 2, line_rows + 2 * streams + 1, LANES), f32),
            pltpu.VMEM((2, 2, dp * seq * (cpd + 1), LANES), f32),
            pltpu.VMEM((dp * seq, 2 * cpd, tokens), bf16),
            pltpu.SemaphoreType.DMA((parts, 2)),
        ),
        specs=([pl.BlockSpec(memory_space=pltpu.VMEM)] * 3, anywhere),
    )(got, taps, ready)
    back = lax.all_to_all(made, both, split_axis=0, concat_axis=0, tiled=True)
    lags = call(
        functools.partial(tap_kernel, inner, float(dp * length) ** -0.5),
        shape((dp, cpd, part), f32),
        (
            pltpu.VMEM((2, slot_rows, LANES), f32),
            pltpu.VMEM((2, slot_rows, LANES), f32),
            pltpu.VMEM((ahead, line_rows, LANES), f32),
            pltpu.VMEM((ahead, PACK + blocks * streams, LANES), f32),
            pltpu.VMEM((ahead, PACK // streams, 2 * blocks * streams, LANES), bf16),
            pltpu.VMEM((ahead, line_rows, LANES), f32),
            pltpu.VMEM((ahead, blocks * 9, LANES), f32),
            pltpu.VMEM((cpd * (blocks + 1), LANES), f32),
        ),
        flops=1 << 30,
    )(got)
    grad_filter = exchange(lags, "dp").reshape(segments, per, part)
    grad_signal, grad_gate = call(
        functools.partial(receive_kernel, edge),
        (shape((tokens, channels), bf16), shape((tokens, channels), bf16)),
    )(back, grad_out[0])
    return (grad_signal[None], grad_gate[None], grad_filter)


def solution(mesh):
    tokens = P("dp", "seq", None)
    taps = P(None, "seq", "dp")
    return jax.shard_map(
        on_device,
        mesh=mesh,
        in_specs=(tokens, tokens, tokens, taps),
        out_specs=(tokens, tokens, taps),
        check_vma=False,
    )
```

```python
import functools

import jax
import jax.numpy as jnp
from jax import lax
from jax.experimental import pallas as pl
from jax.experimental.pallas import tpu as pltpu
from jax.sharding import PartitionSpec as P

LANES = 128
PACK = 16
AHEAD = 2
NEAR = 2
bf16 = jnp.bfloat16
f32 = jnp.float32


def iota(shape, axis):
    return lax.broadcasted_iota(jnp.int32, shape, axis)


def flip_matrix(size, dtype):
    hit = iota((size, size), 0) + iota((size, size), 1) == size - 1
    return jnp.where(hit, 1.0, 0.0).astype(dtype)


def times(a, b):
    return jnp.dot(a, b, preferred_element_type=f32)


def gather_rows(parts):
    return parts[0] if len(parts) == 1 else jnp.concatenate(parts, axis=0)


def send_kernel(sizes, out_grad, gate, signal, sent, grads, gates, signals, made, arrived, left):
    dp, seq, per, spd = sizes
    width = per * seq * spd
    pairs = ((signal, signals), (out_grad, grads), (gate, gates))
    coming = [
        pltpu.make_async_copy(source, held, arrived.at[k]) for k, (source, held) in enumerate(pairs)
    ]
    going = [
        pltpu.make_async_copy(made.at[pl.ds(p * seq, seq)], sent.at[pl.ds(p * seq, seq)], left.at[p])
        for p in range(dp)
    ]
    for copy in coming:
        copy.start()
    flip = flip_matrix(grads.shape[0], bf16)
    for p in range(dp):
        at = pl.ds(p * width, width)
        if p == 0:
            for copy in coming:
                copy.wait()
        scaled = (grads[:, at].astype(f32) * gates[:, at].astype(f32)).T
        scaled = times(scaled.astype(bf16), flip)
        plain = signals[:, at].astype(f32).T
        for q in range(seq):
            parts = []
            for value in (scaled, plain):
                for s in range(spd):
                    begin = (s * seq + q) * per
                    parts.append(value[begin : begin + per])
            made[p * seq + q] = gather_rows(parts).astype(bf16)
        going[p].start()
    for copy in going:
        copy.wait()


def receive_kernel(sizes, got, out_grad, grad_signal, grad_gate):
    dp, seq, per, spd = sizes
    width = per * seq
    cpd = per * spd
    flip = flip_matrix(got.shape[2], bf16)
    for p in range(dp):
        for s in range(spd):
            begin = (p * spd + s) * width
            turned = []
            for t in range(2):
                low = t * cpd + s * per
                block = got[p * seq : (p + 1) * seq].astype(f32)
                block = gather_rows([block[q, low : low + per] for q in range(seq)])
                turned.append((times(block.astype(bf16), flip) if t else block).T)
            grad = out_grad[:, begin : begin + width].astype(f32)
            grad_gate[:, begin : begin + width] = (grad * turned[0]).astype(bf16)
            grad_signal[:, begin : begin + width] = turned[1].astype(bf16)


def slots(b, seq, pitch, first=1):
    return (b * (seq + 1) + first) * pitch


def clear_slots(dp, seq, pitch, held):
    for b in range(dp):
        for half in range(held.shape[0]):
            held[half, pl.ds(slots(b, seq, pitch, 0), pitch), :] = jnp.zeros((pitch, LANES), f32)


def put(held, half, at, value):
    held[half, pl.ds(at, value.shape[0]), :] = value[:, half * LANES : (half + 1) * LANES]


def stage(dp, seq, cpd, got, plain, turned):
    pitch = cpd + 1
    for b in range(dp):
        for q in range(seq):
            value = got[b * seq + q].astype(f32)
            for half in range(2):
                put(plain, half, slots(b, seq, pitch) + q * pitch, value[cpd:])
                put(turned, half, slots(b, seq, pitch) + (seq - 1 - q) * pitch, value[:cpd])


def skew(value):
    return pltpu.roll(value, 0, 1, stride=1, stride_axis=0)


def filter_windows(taps, c, seq, lower, store):
    per_part = taps.shape[2]
    small = LANES // 2
    before = jnp.zeros((small, LANES), bf16)
    for d in range(2 * seq):
        row = taps[d // per_part, c, pl.ds(d % per_part, 1), :]
        now = skew(jnp.broadcast_to(row, (small, LANES))).astype(bf16)
        store(d % 2, pl.ds((d // 2) * small, small), jnp.where(lower, now, before))
        before = now


def window_kernel(seq, taps, made):
    small = LANES // 2
    lower = iota((small, LANES), 1) >= iota((small, LANES), 0)

    def channel(c, carry):
        def store(k, rows, value):
            made[c, k, rows, :] = value

        filter_windows(taps, c, seq, lower, store)
        return carry

    lax.fori_loop(0, made.shape[0], channel, 0)


def mix_kernel(sizes, got, taps, ready, made, plain, turned, line, shifted, windows, result, out, done, left):
    dp, seq, cpd = sizes
    tokens = got.shape[2]
    streams = 2 * dp
    small = LANES // 2
    quarters = tokens // small
    group = quarters * streams
    size = seq * group
    pitch = cpd + 1
    ahead = line.shape[0]

    held = (plain, turned)
    stage(dp, seq, cpd, got, plain, turned)
    for one in held:
        clear_slots(dp, seq, pitch, one)
    for u in range(ahead):
        shifted[u, :size] = jnp.zeros((size, LANES), bf16)
        result[u, 1, : 2 * streams + 1] = jnp.zeros((2 * streams + 1, LANES), f32)
    lower = iota((small, LANES), 1) >= iota((small, LANES), 0)
    low = iota((seq, LANES), 1) < small
    order = [(k, b, half) for k in range(2) for b in range(dp) for half in range(2)]

    def build(c, u, early=False):
        for kind, b, half in order:
            stream = kind * dp + b
            here = held[kind][half, pl.ds(slots(b, seq, pitch) + c, seq, stride=pitch), :]
            behind = held[kind][half, pl.ds(slots(b, seq, pitch, 0) + c, seq, stride=pitch), :]
            crossed = pltpu.roll(jnp.where(low, behind, here), small, 1)
            to = 2 * half * streams + stream
            line[u, pl.ds(to, seq, stride=group + 1), :] = jnp.where(low, here, crossed)
            line[u, pl.ds(to + streams, seq, stride=group + 1), :] = jnp.where(low, crossed, behind)
        for q in range(seq):
            shifted[u, size + q * group : size + (q + 1) * group] = line[u, pl.ds(q * (group + 1), group), :].astype(bf16)
        if not early:

            def store(k, rows, value):
                windows[u, k, rows, :] = value

            filter_windows(taps, c, seq, lower, store)

    def apply(c, u, early=False):
        deep = seq * small // 2
        sums = []
        for which in range(2):
            blocks = []
            count = size >> which
            for f in range(which * seq // 4, (which + 1) * seq // 4):
                blocks.append(shifted[u, pl.ds(2 * size - count - 2 * f * group, count), :])
            source, at = (ready, c) if early else (windows, u)
            tiles = [source[at, k, pl.ds(which * deep, deep), :] for k in range(2)]
            sums.append(times(jnp.concatenate(blocks, axis=1), jnp.concatenate(tiles, axis=1)))
        total = jnp.concatenate([sums[0][: size // 2], sums[0][size // 2 :] + sums[1]], axis=0)
        rows = 2 * streams
        late = jnp.concatenate([jnp.zeros((rows, LANES), f32), total[: size - rows, LANES:]], axis=0)
        total = total[:, :LANES] + late
        for k in range(2 * seq):
            result[u, k % 2, pl.ds((k // 2 + 1) * (rows + 1), rows), :] = total[k * rows : (k + 1) * rows]
        for kind, b, half in order:
            stream = kind * dp + b
            first = rows + 1 + stream
            even = result[u, half, pl.ds(first, seq, stride=rows + 1), :]
            here = result[u, half, pl.ds(first + streams, seq, stride=rows + 1), :]
            at = first + streams if half else stream + streams
            behind = result[u, 1 - half, pl.ds(at, seq, stride=rows + 1), :]
            value = even + pltpu.roll(jnp.where(low, here, behind), small, 1)
            out[kind, half, pl.ds(b * seq * pitch + c, seq, stride=pitch), :] = value

    parts = left.shape[0]
    each = cpd // parts

    def going(part, kind):
        to = pl.ds(kind * cpd + part * each, each)
        return pltpu.make_async_copy(done.at[:, to, :], made.at[:, to, :], left.at[part, kind])

    def finish(part):
        for kind in range(2):
            to = pl.ds(kind * cpd + part * each, each)
            for b in range(dp):
                for q in range(seq):
                    at = pl.ds((b * seq + q) * pitch + part * each, each)
                    value = jnp.concatenate([out[kind, half, at, :] for half in range(2)], axis=1)
                    done[b * seq + (seq - 1 - q if kind else q), to, :] = value.astype(bf16)
            going(part, kind).start()

    near = ahead // 2
    pairs = cpd // ahead

    def each_of(work, first, side, early=False):
        for u in range(near):
            work(first + u, side * near + u, early)

    def step(k, carry):
        if parts > 1:
            pl.when(k == pairs // parts)(lambda: finish(0))
        each_of(build, k * ahead + near, 1)
        each_of(apply, k * ahead, 0)
        each_of(build, k * ahead + ahead, 0)
        each_of(apply, k * ahead + near, 1)
        return carry

    begin = ready.shape[0] // ahead
    each_of(build, 0, 0, begin > 0)
    if begin:
        each_of(build, near, 1, True)
        each_of(apply, 0, 0, True)
        each_of(build, ahead, 0)
        each_of(apply, near, 1, True)
    lax.fori_loop(begin, pairs - 1, step, 0)
    each_of(build, cpd - near, 1)
    each_of(apply, cpd - ahead, 0)
    each_of(apply, cpd - near, 1)
    finish(parts - 1)
    for part in range(parts):
        for kind in range(2):
            going(part, kind).wait()


def tap_kernel(sizes, factor, got, made, mirrored, turned, line, flat, shifted, square, partial, lags):
    dp, seq, cpd = sizes
    streams = 2 * dp
    blocks = 2 * seq
    rows = 2 * streams
    size = seq * rows
    small = LANES // 2
    pitch = cpd + 1
    ahead = line.shape[0]
    clear_slots(dp, seq, pitch, turned)
    for b in range(dp):
        for q in range(seq):
            value = got[b * seq + q].astype(f32)
            to = slots(b, seq, pitch) + (seq - 1 - q) * pitch
            for half in range(2):
                put(turned, half, to, value[:cpd])
                at = pl.ds(to, cpd)
                mirrored[1 - half, at, :] = value[cpd:, half * LANES : (half + 1) * LANES]
    for u in range(ahead):
        flat[u, :PACK] = jnp.zeros((PACK, LANES), f32)
        for k in range(PACK // streams):
            shifted[u, k, :size] = jnp.zeros((size, LANES), bf16)
    low = iota((seq, LANES), 1) < small
    lower = iota((small, LANES), 1) >= iota((small, LANES), 0)

    def channel(c, u):
        for b in range(dp):
            here = [turned[half, pl.ds(slots(b, seq, pitch) + c, seq, stride=pitch), :] for half in range(2)]
            behind = [turned[1, pl.ds(slots(b, seq, pitch, 0) + c, seq, stride=pitch), :], here[0]]
            for half in range(2):
                late = pltpu.roll(jnp.where(low, here[half], behind[half]), small, 1)
                line[u, pl.ds(half * streams + b, seq, stride=rows + 1), :] = here[half]
                line[u, pl.ds(half * streams + dp + b, seq, stride=rows + 1), :] = late
                value = mirrored[half, pl.ds(slots(b, seq, pitch) + c, seq, stride=pitch), :]
                square[u, pl.ds(half * streams + b, seq, stride=rows + 1), :] = value
                square[u, pl.ds(half * streams + dp + b, seq, stride=rows + 1), :] = pltpu.roll(value, small, 1)
        for q in range(seq):
            flat[u, PACK + q * rows : PACK + (q + 1) * rows] = line[u, pl.ds(q * (rows + 1), rows), :]
        for k in range(PACK // streams):
            shifted[u, k, size:] = flat[u, pl.ds(PACK - k * streams, size), :].astype(bf16)
        wide = jnp.concatenate([square[u, pl.ds(q * (rows + 1), rows), :] for q in range(seq)], axis=0)
        left = wide.T[:small].astype(bf16)
        before = jnp.zeros((small, LANES), f32)
        for pair in range(blocks // 2):
            right = []
            for at in (2 * pair + 1, 2 * pair + 2):
                k = -at % (PACK // streams)
                right.append(shifted[u, k, pl.ds((at + k) * streams, size), :])
            product = times(left, jnp.concatenate(right, axis=1))
            for k in range(2):
                now = skew(product[:, k * LANES : (k + 1) * LANES])
                value = jnp.where(lower, now, before)
                before = now
                value = jnp.sum(value.reshape(small // 8, 8, LANES), axis=0)
                partial[u, pl.ds((2 * pair + k) * 9, 8), :] = value
        total = partial[u, pl.ds(0, blocks, stride=9), :]
        for j in range(1, 8):
            total = total + partial[u, pl.ds(j, blocks, stride=9), :]
        lags[pl.ds(c * (blocks + 1), blocks), :] = total * factor

    def step(i, carry):
        for u in range(ahead):
            channel(i * ahead + u, u)
        return carry

    lax.fori_loop(0, cpd // ahead, step, 0)
    flip = flip_matrix(LANES, f32)
    for c in range(cpd):
        at = pl.ds(c * (blocks + 1), blocks)
        lags[at, :] = jnp.dot(lags[at, :], flip, preferred_element_type=f32, precision=lax.Precision.HIGHEST)
    per_part = blocks // made.shape[0]
    for k in range(blocks):
        column = pl.ds((k % per_part) * LANES, LANES)
        made[k // per_part, :, column] = lags[pl.ds(blocks - 1 - k, cpd, stride=blocks + 1), :]


def exchange(blocks, axis):
    size = blocks.shape[0]
    me = lax.axis_index(axis)
    own = lax.dynamic_index_in_dim(blocks, me, 0, True)
    result = lax.dynamic_update_slice_in_dim(jnp.zeros_like(blocks), own, me, 0)
    for k in range(1, size):
        part = lax.dynamic_index_in_dim(blocks, (me + k) % size, 0, True)
        part = lax.ppermute(part, axis, [(i, (i + k) % size) for i in range(size)])
        result = lax.dynamic_update_slice_in_dim(result, part, (me - k) % size, 0)
    return result


def call(kernel, out_shape, scratch=(), flops=0, limit=24, specs=None):
    extra = {} if specs is None else dict(in_specs=specs[0], out_specs=specs[1])
    return pl.pallas_call(
        kernel,
        out_shape=out_shape,
        scratch_shapes=list(scratch),
        cost_estimate=pl.CostEstimate(flops=flops, bytes_accessed=1 << 20, transcendentals=0),
        compiler_params=pltpu.CompilerParams(vmem_limit_bytes=limit << 20),
        **extra,
    )


def on_device(grad_out, gate, signal, filters):
    shape = jax.ShapeDtypeStruct
    dp, seq = lax.axis_size("dp"), lax.axis_size("seq")
    tokens, channels = grad_out.shape[1:]
    segments, per, part = filters.shape
    spd = segments // dp
    cpd = spd * per
    length = tokens * seq
    blocks = length // LANES
    streams = 2 * dp
    group = 4 * streams
    slot_rows = dp * (seq + 1) * (cpd + 1)
    line_rows = seq * (2 * streams + 1)
    ahead = AHEAD if cpd % AHEAD == 0 else 1
    many = 2 * NEAR if cpd % (2 * NEAR) == 0 else 2
    both = ("dp", "seq")
    taps = exchange(filters.reshape(dp, cpd, part // LANES, LANES), "dp")
    edge = (dp, seq, per, spd)
    anywhere = pl.BlockSpec(memory_space=pl.ANY)
    sent = call(
        functools.partial(send_kernel, edge),
        shape((dp * seq, 2 * cpd, tokens), bf16),
        (
            pltpu.VMEM((tokens, channels), bf16),
            pltpu.VMEM((tokens, channels), bf16),
            pltpu.VMEM((tokens, channels), bf16),
            pltpu.VMEM((dp * seq, 2 * cpd, tokens), bf16),
            pltpu.SemaphoreType.DMA((3,)),
            pltpu.SemaphoreType.DMA((dp,)),
        ),
        limit=63,
        specs=([anywhere] * 3, anywhere),
    )(grad_out[0], gate[0], signal[0])
    got = lax.all_to_all(sent, both, split_axis=0, concat_axis=0, tiled=True)
    inner = (dp, seq, cpd)
    pairs = cpd // many
    ready = call(
        functools.partial(window_kernel, seq),
        shape((many if pairs > 2 else 1, 2, seq * LANES // 2, LANES), bf16),
        flops=1 << 30,
        specs=([pl.BlockSpec(memory_space=pltpu.VMEM)], pl.BlockSpec(memory_space=pltpu.VMEM)),
    )(taps)
    parts = 2 if cpd % (4 * many) == 0 else 1
    made = call(
        functools.partial(mix_kernel, inner),
        shape((dp * seq, 2 * cpd, tokens), bf16),
        (
            pltpu.VMEM((2, slot_rows, LANES), f32),
            pltpu.VMEM((2, slot_rows, LANES), f32),
            pltpu.VMEM((many, seq * (group + 1), LANES), f32),
            pltpu.VMEM((many, 2 * seq * group, LANES), bf16),
            pltpu.VMEM((many, 2, seq * LANES // 2, LANES), bf16),
            pltpu.VMEM((many, 2, line_rows + 2 * streams + 1, LANES), f32),
            pltpu.VMEM((2, 2, dp * seq * (cpd + 1), LANES), f32),
            pltpu.VMEM((dp * seq, 2 * cpd, tokens), bf16),
            pltpu.SemaphoreType.DMA((parts, 2)),
        ),
        specs=([pl.BlockSpec(memory_space=pltpu.VMEM)] * 3, anywhere),
    )(got, taps, ready)
    back = lax.all_to_all(made, both, split_axis=0, concat_axis=0, tiled=True)
    lags = call(
        functools.partial(tap_kernel, inner, float(dp * length) ** -0.5),
        shape((dp, cpd, part), f32),
        (
            pltpu.VMEM((2, slot_rows, LANES), f32),
            pltpu.VMEM((2, slot_rows, LANES), f32),
            pltpu.VMEM((ahead, line_rows, LANES), f32),
            pltpu.VMEM((ahead, PACK + blocks * streams, LANES), f32),
            pltpu.VMEM((ahead, PACK // streams, 2 * blocks * streams, LANES), bf16),
            pltpu.VMEM((ahead, line_rows, LANES), f32),
            pltpu.VMEM((ahead, blocks * 9, LANES), f32),
            pltpu.VMEM((cpd * (blocks + 1), LANES), f32),
        ),
        flops=1 << 30,
    )(got)
    grad_filter = exchange(lags, "dp").reshape(segments, per, part)
    grad_signal, grad_gate = call(
        functools.partial(receive_kernel, edge),
        (shape((tokens, channels), bf16), shape((tokens, channels), bf16)),
    )(back, grad_out[0])
    return (grad_signal[None], grad_gate[None], grad_filter)


def solution(mesh):
    tokens = P("dp", "seq", None)
    taps = P(None, "seq", "dp")
    return jax.shard_map(
        on_device,
        mesh=mesh,
        in_specs=(tokens, tokens, tokens, taps),
        out_specs=(tokens, tokens, taps),
        check_vma=False,
    )
```

```python
import functools

import jax
import jax.numpy as jnp
from jax import lax
from jax.experimental import pallas as pl
from jax.experimental.pallas import tpu as pltpu
from jax.sharding import PartitionSpec as P

LANES = 128
PACK = 16
AHEAD = 2
NEAR = 2
bf16 = jnp.bfloat16
f32 = jnp.float32


def iota(shape, axis):
    return lax.broadcasted_iota(jnp.int32, shape, axis)


def flip_matrix(size, dtype):
    hit = iota((size, size), 0) + iota((size, size), 1) == size - 1
    return jnp.where(hit, 1.0, 0.0).astype(dtype)


def times(a, b):
    return jnp.dot(a, b, preferred_element_type=f32)


def gather_rows(parts):
    return parts[0] if len(parts) == 1 else jnp.concatenate(parts, axis=0)


def send_kernel(sizes, out_grad, gate, signal, sent, grads, gates, signals, made, arrived, left):
    dp, seq, per, spd = sizes
    width = per * seq * spd
    pairs = ((signal, signals), (out_grad, grads), (gate, gates))
    coming = [
        pltpu.make_async_copy(source, held, arrived.at[k]) for k, (source, held) in enumerate(pairs)
    ]
    going = [
        pltpu.make_async_copy(made.at[pl.ds(p * seq, seq)], sent.at[pl.ds(p * seq, seq)], left.at[p])
        for p in range(dp)
    ]
    for copy in coming:
        copy.start()
    flip = flip_matrix(grads.shape[0], bf16)
    coming[0].wait()
    turned = [signals[:, pl.ds(p * width, width)].astype(f32).T for p in range(dp)]
    for copy in coming[1:]:
        copy.wait()
    for p in range(dp):
        at = pl.ds(p * width, width)
        scaled = (grads[:, at].astype(f32) * gates[:, at].astype(f32)).T
        scaled = times(scaled.astype(bf16), flip)
        plain = turned[p]
        for q in range(seq):
            parts = []
            for value in (scaled, plain):
                for s in range(spd):
                    begin = (s * seq + q) * per
                    parts.append(value[begin : begin + per])
            made[p * seq + q] = gather_rows(parts).astype(bf16)
        going[p].start()
    for copy in going:
        copy.wait()


def receive_kernel(sizes, got, out_grad, grad_signal, grad_gate):
    dp, seq, per, spd = sizes
    width = per * seq
    cpd = per * spd
    flip = flip_matrix(got.shape[2], bf16)
    for p in range(dp):
        for s in range(spd):
            begin = (p * spd + s) * width
            turned = []
            for t in range(2):
                low = t * cpd + s * per
                block = got[p * seq : (p + 1) * seq].astype(f32)
                block = gather_rows([block[q, low : low + per] for q in range(seq)])
                turned.append((times(block.astype(bf16), flip) if t else block).T)
            grad = out_grad[:, begin : begin + width].astype(f32)
            grad_gate[:, begin : begin + width] = (grad * turned[0]).astype(bf16)
            grad_signal[:, begin : begin + width] = turned[1].astype(bf16)


def slots(b, seq, pitch, first=1):
    return (b * (seq + 1) + first) * pitch


def clear_slots(dp, seq, pitch, held):
    for b in range(dp):
        for half in range(held.shape[0]):
            held[half, pl.ds(slots(b, seq, pitch, 0), pitch), :] = jnp.zeros((pitch, LANES), f32)


def put(held, half, at, value):
    held[half, pl.ds(at, value.shape[0]), :] = value[:, half * LANES : (half + 1) * LANES]


def stage(dp, seq, cpd, got, plain, turned):
    pitch = cpd + 1
    for b in range(dp):
        for q in range(seq):
            value = got[b * seq + q].astype(f32)
            for half in range(2):
                put(plain, half, slots(b, seq, pitch) + q * pitch, value[cpd:])
                put(turned, half, slots(b, seq, pitch) + (seq - 1 - q) * pitch, value[:cpd])


def skew(value):
    return pltpu.roll(value, 0, 1, stride=1, stride_axis=0)


def filter_windows(taps, c, seq, lower, store):
    per_part = taps.shape[2]
    small = LANES // 2
    before = jnp.zeros((small, LANES), bf16)
    for d in range(2 * seq):
        row = taps[d // per_part, c, pl.ds(d % per_part, 1), :]
        now = skew(jnp.broadcast_to(row, (small, LANES))).astype(bf16)
        store(d % 2, pl.ds((d // 2) * small, small), jnp.where(lower, now, before))
        before = now


def window_kernel(seq, taps, made):
    small = LANES // 2
    lower = iota((small, LANES), 1) >= iota((small, LANES), 0)

    def channel(c, carry):
        def store(k, rows, value):
            made[c, k, rows, :] = value

        filter_windows(taps, c, seq, lower, store)
        return carry

    lax.fori_loop(0, made.shape[0], channel, 0)


def mix_kernel(sizes, got, taps, ready, made, plain, turned, line, shifted, windows, result, out, done, left):
    dp, seq, cpd = sizes
    tokens = got.shape[2]
    streams = 2 * dp
    small = LANES // 2
    quarters = tokens // small
    group = quarters * streams
    size = seq * group
    pitch = cpd + 1
    ahead = line.shape[0]

    held = (plain, turned)
    stage(dp, seq, cpd, got, plain, turned)
    for one in held:
        clear_slots(dp, seq, pitch, one)
    for u in range(ahead):
        shifted[u, :size] = jnp.zeros((size, LANES), bf16)
        result[u, 1, : 2 * streams + 1] = jnp.zeros((2 * streams + 1, LANES), f32)
    lower = iota((small, LANES), 1) >= iota((small, LANES), 0)
    low = iota((seq, LANES), 1) < small
    order = [(k, b, half) for k in range(2) for b in range(dp) for half in range(2)]

    def build(c, u, early=False):
        for kind, b, half in order:
            stream = kind * dp + b
            here = held[kind][half, pl.ds(slots(b, seq, pitch) + c, seq, stride=pitch), :]
            behind = held[kind][half, pl.ds(slots(b, seq, pitch, 0) + c, seq, stride=pitch), :]
            crossed = pltpu.roll(jnp.where(low, behind, here).astype(bf16), small, 1).astype(f32)
            to = 2 * half * streams + stream
            line[u, pl.ds(to, seq, stride=group + 1), :] = jnp.where(low, here, crossed)
            line[u, pl.ds(to + streams, seq, stride=group + 1), :] = jnp.where(low, crossed, behind)
        for q in range(seq):
            shifted[u, size + q * group : size + (q + 1) * group] = line[u, pl.ds(q * (group + 1), group), :].astype(bf16)
        if not early:

            def store(k, rows, value):
                windows[u, k, rows, :] = value

            filter_windows(taps, c, seq, lower, store)

    def apply(c, u, early=False):
        deep = seq * small // 2
        sums = []
        for which in range(2):
            blocks = []
            count = size >> which
            for f in range(which * seq // 4, (which + 1) * seq // 4):
                blocks.append(shifted[u, pl.ds(2 * size - count - 2 * f * group, count), :])
            source, at = (ready, c) if early else (windows, u)
            tiles = [source[at, k, pl.ds(which * deep, deep), :] for k in range(2)]
            sums.append(times(jnp.concatenate(blocks, axis=1), jnp.concatenate(tiles, axis=1)))
        total = jnp.concatenate([sums[0][: size // 2], sums[0][size // 2 :] + sums[1]], axis=0)
        rows = 2 * streams
        late = jnp.concatenate([jnp.zeros((rows, LANES), f32), total[: size - rows, LANES:]], axis=0)
        total = total[:, :LANES] + late
        for k in range(2 * seq):
            result[u, k % 2, pl.ds((k // 2 + 1) * (rows + 1), rows), :] = total[k * rows : (k + 1) * rows]
        for kind, b, half in order:
            stream = kind * dp + b
            first = rows + 1 + stream
            even = result[u, half, pl.ds(first, seq, stride=rows + 1), :]
            here = result[u, half, pl.ds(first + streams, seq, stride=rows + 1), :]
            at = first + streams if half else stream + streams
            behind = result[u, 1 - half, pl.ds(at, seq, stride=rows + 1), :]
            value = even + pltpu.roll(jnp.where(low, here, behind), small, 1)
            out[kind, half, pl.ds(b * seq * pitch + c, seq, stride=pitch), :] = value

    parts = left.shape[0]
    each = cpd // parts

    def going(part, kind):
        to = pl.ds(kind * cpd + part * each, each)
        return pltpu.make_async_copy(done.at[:, to, :], made.at[:, to, :], left.at[part, kind])

    def finish(part):
        for kind in range(2):
            to = pl.ds(kind * cpd + part * each, each)
            for b in range(dp):
                for q in range(seq):
                    at = pl.ds((b * seq + q) * pitch + part * each, each)
                    value = jnp.concatenate([out[kind, half, at, :] for half in range(2)], axis=1)
                    done[b * seq + (seq - 1 - q if kind else q), to, :] = value.astype(bf16)
            going(part, kind).start()

    near = ahead // 2
    pairs = cpd // ahead

    def each_of(work, first, side, early=False):
        for u in range(near):
            work(first + u, side * near + u, early)

    def step(k, carry):
        if parts > 1:
            pl.when(k == pairs // parts)(lambda: finish(0))
        each_of(build, k * ahead + near, 1)
        each_of(apply, k * ahead, 0)
        each_of(build, k * ahead + ahead, 0)
        each_of(apply, k * ahead + near, 1)
        return carry

    begin = ready.shape[0] // ahead
    each_of(build, 0, 0, begin > 0)
    if begin:
        each_of(build, near, 1, True)
        each_of(apply, 0, 0, True)
        each_of(build, ahead, 0)
        each_of(apply, near, 1, True)
    lax.fori_loop(begin, pairs - 1, step, 0)
    each_of(build, cpd - near, 1)
    each_of(apply, cpd - ahead, 0)
    each_of(apply, cpd - near, 1)
    finish(parts - 1)
    for part in range(parts):
        for kind in range(2):
            going(part, kind).wait()


def tap_kernel(sizes, factor, got, made, mirrored, turned, line, flat, shifted, square, partial, lags):
    dp, seq, cpd = sizes
    streams = 2 * dp
    blocks = 2 * seq
    rows = 2 * streams
    size = seq * rows
    small = LANES // 2
    pitch = cpd + 1
    ahead = line.shape[0]
    clear_slots(dp, seq, pitch, turned)
    for b in range(dp):
        for q in range(seq):
            value = got[b * seq + q].astype(f32)
            to = slots(b, seq, pitch) + (seq - 1 - q) * pitch
            for half in range(2):
                put(turned, half, to, value[:cpd])
                at = pl.ds(to, cpd)
                mirrored[1 - half, at, :] = value[cpd:, half * LANES : (half + 1) * LANES]
    for u in range(ahead):
        flat[u, :PACK] = jnp.zeros((PACK, LANES), f32)
        for k in range(PACK // streams):
            shifted[u, k, :size] = jnp.zeros((size, LANES), bf16)
    low = iota((seq, LANES), 1) < small
    lower = iota((small, LANES), 1) >= iota((small, LANES), 0)

    def channel(c, u):
        for b in range(dp):
            here = [turned[half, pl.ds(slots(b, seq, pitch) + c, seq, stride=pitch), :] for half in range(2)]
            behind = [turned[1, pl.ds(slots(b, seq, pitch, 0) + c, seq, stride=pitch), :], here[0]]
            for half in range(2):
                late = pltpu.roll(jnp.where(low, here[half], behind[half]), small, 1)
                line[u, pl.ds(half * streams + b, seq, stride=rows + 1), :] = here[half]
                line[u, pl.ds(half * streams + dp + b, seq, stride=rows + 1), :] = late
                value = mirrored[half, pl.ds(slots(b, seq, pitch) + c, seq, stride=pitch), :]
                square[u, pl.ds(half * streams + b, seq, stride=rows + 1), :] = value
                square[u, pl.ds(half * streams + dp + b, seq, stride=rows + 1), :] = pltpu.roll(value, small, 1)
        for q in range(seq):
            flat[u, PACK + q * rows : PACK + (q + 1) * rows] = line[u, pl.ds(q * (rows + 1), rows), :]
        for k in range(PACK // streams):
            shifted[u, k, size:] = flat[u, pl.ds(PACK - k * streams, size), :].astype(bf16)
        wide = jnp.concatenate([square[u, pl.ds(q * (rows + 1), rows), :] for q in range(seq)], axis=0)
        left = wide.T[:small].astype(bf16)
        before = jnp.zeros((small, LANES), f32)
        for pair in range(blocks // 2):
            right = []
            for at in (2 * pair + 1, 2 * pair + 2):
                k = -at % (PACK // streams)
                right.append(shifted[u, k, pl.ds((at + k) * streams, size), :])
            product = times(left, jnp.concatenate(right, axis=1))
            for k in range(2):
                now = skew(product[:, k * LANES : (k + 1) * LANES])
                value = jnp.where(lower, now, before)
                before = now
                value = jnp.sum(value.reshape(small // 8, 8, LANES), axis=0)
                partial[u, pl.ds((2 * pair + k) * 9, 8), :] = value
        total = partial[u, pl.ds(0, blocks, stride=9), :]
        for j in range(1, 8):
            total = total + partial[u, pl.ds(j, blocks, stride=9), :]
        lags[pl.ds(c * (blocks + 1), blocks), :] = total * factor

    def step(i, carry):
        for u in range(ahead):
            channel(i * ahead + u, u)
        return carry

    lax.fori_loop(0, cpd // ahead, step, 0)
    flip = flip_matrix(LANES, f32)
    for c in range(cpd):
        at = pl.ds(c * (blocks + 1), blocks)
        lags[at, :] = jnp.dot(lags[at, :], flip, preferred_element_type=f32, precision=lax.Precision.HIGHEST)
    per_part = blocks // made.shape[0]
    for k in range(blocks):
        column = pl.ds((k % per_part) * LANES, LANES)
        made[k // per_part, :, column] = lags[pl.ds(blocks - 1 - k, cpd, stride=blocks + 1), :]


def exchange(blocks, axis):
    size = blocks.shape[0]
    me = lax.axis_index(axis)
    own = lax.dynamic_index_in_dim(blocks, me, 0, True)
    result = lax.dynamic_update_slice_in_dim(jnp.zeros_like(blocks), own, me, 0)
    for k in range(1, size):
        part = lax.dynamic_index_in_dim(blocks, (me + k) % size, 0, True)
        part = lax.ppermute(part, axis, [(i, (i + k) % size) for i in range(size)])
        result = lax.dynamic_update_slice_in_dim(result, part, (me - k) % size, 0)
    return result


def call(kernel, out_shape, scratch=(), flops=0, limit=24, specs=None):
    extra = {} if specs is None else dict(in_specs=specs[0], out_specs=specs[1])
    return pl.pallas_call(
        kernel,
        out_shape=out_shape,
        scratch_shapes=list(scratch),
        cost_estimate=pl.CostEstimate(flops=flops, bytes_accessed=1 << 20, transcendentals=0),
        compiler_params=pltpu.CompilerParams(vmem_limit_bytes=limit << 20),
        **extra,
    )


def on_device(grad_out, gate, signal, filters):
    shape = jax.ShapeDtypeStruct
    dp, seq = lax.axis_size("dp"), lax.axis_size("seq")
    tokens, channels = grad_out.shape[1:]
    segments, per, part = filters.shape
    spd = segments // dp
    cpd = spd * per
    length = tokens * seq
    blocks = length // LANES
    streams = 2 * dp
    group = 4 * streams
    slot_rows = dp * (seq + 1) * (cpd + 1)
    line_rows = seq * (2 * streams + 1)
    ahead = AHEAD if cpd % AHEAD == 0 else 1
    many = 2 * NEAR if cpd % (2 * NEAR) == 0 else 2
    both = ("dp", "seq")
    taps = exchange(filters.reshape(dp, cpd, part // LANES, LANES), "dp")
    edge = (dp, seq, per, spd)
    anywhere = pl.BlockSpec(memory_space=pl.ANY)
    sent = call(
        functools.partial(send_kernel, edge),
        shape((dp * seq, 2 * cpd, tokens), bf16),
        (
            pltpu.VMEM((tokens, channels), bf16),
            pltpu.VMEM((tokens, channels), bf16),
            pltpu.VMEM((tokens, channels), bf16),
            pltpu.VMEM((dp * seq, 2 * cpd, tokens), bf16),
            pltpu.SemaphoreType.DMA((3,)),
            pltpu.SemaphoreType.DMA((dp,)),
        ),
        limit=63,
        specs=([anywhere] * 3, anywhere),
    )(grad_out[0], gate[0], signal[0])
    got = lax.all_to_all(sent, both, split_axis=0, concat_axis=0, tiled=True)
    inner = (dp, seq, cpd)
    pairs = cpd // many
    ready = call(
        functools.partial(window_kernel, seq),
        shape((many if pairs > 2 else 1, 2, seq * LANES // 2, LANES), bf16),
        flops=1 << 30,
        specs=([pl.BlockSpec(memory_space=pltpu.VMEM)], pl.BlockSpec(memory_space=pltpu.VMEM)),
    )(taps)
    parts = 2 if cpd % (4 * many) == 0 else 1
    made = call(
        functools.partial(mix_kernel, inner),
        shape((dp * seq, 2 * cpd, tokens), bf16),
        (
            pltpu.VMEM((2, slot_rows, LANES), f32),
            pltpu.VMEM((2, slot_rows, LANES), f32),
            pltpu.VMEM((many, seq * (group + 1), LANES), f32),
            pltpu.VMEM((many, 2 * seq * group, LANES), bf16),
            pltpu.VMEM((many, 2, seq * LANES // 2, LANES), bf16),
            pltpu.VMEM((many, 2, line_rows + 2 * streams + 1, LANES), f32),
            pltpu.VMEM((2, 2, dp * seq * (cpd + 1), LANES), f32),
            pltpu.VMEM((dp * seq, 2 * cpd, tokens), bf16),
            pltpu.SemaphoreType.DMA((parts, 2)),
        ),
        specs=([pl.BlockSpec(memory_space=pltpu.VMEM)] * 3, anywhere),
    )(got, taps, ready)
    back = lax.all_to_all(made, both, split_axis=0, concat_axis=0, tiled=True)
    lags = call(
        functools.partial(tap_kernel, inner, float(dp * length) ** -0.5),
        shape((dp, cpd, part), f32),
        (
            pltpu.VMEM((2, slot_rows, LANES), f32),
            pltpu.VMEM((2, slot_rows, LANES), f32),
            pltpu.VMEM((ahead, line_rows, LANES), f32),
            pltpu.VMEM((ahead, PACK + blocks * streams, LANES), f32),
            pltpu.VMEM((ahead, PACK // streams, 2 * blocks * streams, LANES), bf16),
            pltpu.VMEM((ahead, line_rows, LANES), f32),
            pltpu.VMEM((ahead, blocks * 9, LANES), f32),
            pltpu.VMEM((cpd * (blocks + 1), LANES), f32),
        ),
        flops=1 << 30,
    )(got)
    grad_filter = exchange(lags, "dp").reshape(segments, per, part)
    grad_signal, grad_gate = call(
        functools.partial(receive_kernel, edge),
        (shape((tokens, channels), bf16), shape((tokens, channels), bf16)),
    )(back, grad_out[0])
    return (grad_signal[None], grad_gate[None], grad_filter)


def solution(mesh):
    tokens = P("dp", "seq", None)
    taps = P(None, "seq", "dp")
    return jax.shard_map(
        on_device,
        mesh=mesh,
        in_specs=(tokens, tokens, tokens, taps),
        out_specs=(tokens, tokens, taps),
        check_vma=False,
    )
```
